32 devices in a mesh: dp: 8 (over y, x, core), tensor: 4 (over z).
Axes of the slice: x: 2, y: 2, z: 4, core: 2. Of those that a mesh axis runs over, the one named last changes fastest.
Arguments:
- noisy_embed: bfloat16 [16384, 16], P(('dp', 'tensor')), may hold values from -6 to 6
- self_cond: bfloat16 [16384, 16], P(('dp', 'tensor')), may hold values from -6 to 6
- cond_flag: int32 [16], P('dp'), may hold values 0 or 1
- timestep: int32 [16], P('dp'), may hold values from 0 to 1023
- in_weight: bfloat16 [32, 768], replicated, may hold values from -1 to 1
- qkv_weight: bfloat16 [3, 768, 768], P(None, None, 'tensor'), may hold values from -0.21875 to 0.21875
- out_weight: bfloat16 [768, 768], P('tensor'), may hold values from -3.5 to 3.5
- up_weight: bfloat16 [768, 3072], P(None, 'tensor'), may hold values from -0.21875 to 0.21875
- up_bias: bfloat16 [3072], P('tensor'), may hold values from -3 to 3
- down_weight: bfloat16 [3072, 768], P('tensor'), may hold values from -0.109375 to 0.109375
- ada_weight: bfloat16 [256, 2304], replicated, may hold values from -0.375 to 0.375
- norm_gain: float32 [768], replicated, may hold values from 0.1 to 1.9
- norm_bias: float32 [768], replicated, may hold values from -3 to 3
- out_grad: float32 [16384, 768], P(('dp', 'tensor')), may hold values from -6 to 6
Outputs:
- result: float32 [16384, 768], P(('dp', 'tensor'))
- grad_noisy: float32 [16384, 16], P(('dp', 'tensor'))
- grad_self: float32 [16384, 16], P(('dp', 'tensor'))
- grad_in_weight: float32 [32, 768], replicated
- grad_qkv_weight: float32 [3, 768, 768], P(None, None, 'tensor')
- grad_out_weight: float32 [768, 768], P('tensor')
- grad_up_weight: float32 [768, 3072], P(None, 'tensor')
- grad_up_bias: float32 [3072], P('tensor')
- grad_down_weight: float32 [3072, 768], P('tensor')
- grad_ada_weight: float32 [256, 2304], replicated
- grad_norm_gain: float32 [768], replicated
- grad_norm_bias: float32 [768], replicated
The draws below stay inside these ranges and needn't reach their ends.
All inputs are finite; a program needn't handle non-finite values. No bound on the sum of `cond_flag` on one device may be relied on, other than what follows from the above.
Results may differ from the reference program's by a relative error of at most 0.017.
Values may be sent and summed in bfloat16 or wider, within the bound.
A program may use at most 128 MiB of HBM per device.

```python
import math
import jax
import jax.numpy as jnp
from jax import lax

D = 768
H = 12
HD = 64
FF = 3072
EMB = 16
TE = 256
LEN = 1024
SEQ_DEV = 2
SEQS = 16
TOKENS = 16384


def with_ends(drawn, rng, low, high):
    spot = [jax.random.randint(jax.random.fold_in(rng, axis), (), 0, length) for axis, length in enumerate(drawn.shape)]
    main_axis = drawn.shape.index(max(drawn.shape))
    beside = spot[:main_axis] + [(spot[main_axis] + 1) % drawn.shape[main_axis]] + spot[main_axis + 1:]
    return drawn.at[tuple(spot)].set(low).at[tuple(beside)].set(high)


def steps_of(rng, extent, pieces, smallest, top_value):
    def one(position, parts):
        draws = jax.random.uniform(jax.random.fold_in(jax.random.fold_in(rng, 6), position), (parts,), jnp.float32, smallest / len(pieces), top_value / len(pieces))
        return jnp.repeat(jnp.exp(draws), extent[position] // parts).reshape((-1,) + (1,) * (len(extent) - position - 1))

    factor_of = one(*pieces[0])
    for cut in pieces[1:]:
        factor_of = factor_of * one(*cut)
    return factor_of


def bell_draw(stream_key, shape, scale, bound, split=(), kind=jnp.bfloat16):
    entries = scale * jax.random.normal(stream_key, shape, jnp.float32)
    if split:
        entries = entries * steps_of(stream_key, shape, split, -0.22, 0.18)
    return jnp.clip(entries, -bound, bound).astype(kind)


def setup_inputs(seed: int = 0) -> dict:
    splits = jax.random.split(jax.random.key(seed), 15)
    noisy_embed = bell_draw(splits[0], (TOKENS, EMB), 1.0, 6.0, ((0, 32),))
    self_cond = bell_draw(splits[1], (TOKENS, EMB), 1.0, 6.0, ((0, 32),))
    cond_flag = with_ends((jax.random.randint(splits[2], (SEQS,), 0, 2) < 1).astype(jnp.int32), jax.random.fold_in(splits[2], 1), 0, 1)
    timestep = with_ends(jax.random.randint(splits[3], (SEQS,), 0, 1024), jax.random.fold_in(splits[3], 1), 0, 1023).astype(jnp.int32)
    in_weight = bell_draw(splits[4], (2 * EMB, D), (2 * EMB) ** -0.5, 1.0)
    qkv_weight = bell_draw(splits[5], (3, D, D), D ** -0.5, 0.21875, ((2, 4),))
    out_weight = bell_draw(splits[6], (D, D), (max(1, 4 * D // LEN)) ** -0.5, 3.5, ((0, 4),))
    up_weight = bell_draw(splits[7], (D, FF), D ** -0.5, 0.21875, ((1, 4),))
    up_bias = bell_draw(splits[8], (FF,), 0.5, 3.0, ((0, 4),))
    down_weight = bell_draw(splits[9], (FF, D), FF ** -0.5, 0.109375, ((0, 4),))
    ada_weight = bell_draw(splits[10], (TE, 3 * D), TE ** -0.5, 0.375)
    norm_gain = jnp.clip(1.0 + 0.18 * jax.random.normal(splits[11], (D,), jnp.float32), 0.1, 1.9)
    norm_bias = bell_draw(splits[12], (D,), 0.5, 3.0, (), jnp.float32)
    out_grad = bell_draw(splits[13], (TOKENS, D), 1.0, 6.0, ((0, 32),), jnp.float32)
    return {"noisy_embed": noisy_embed, "self_cond": self_cond, "cond_flag": cond_flag, "timestep": timestep, "in_weight": in_weight, "qkv_weight": qkv_weight, "out_weight": out_weight, "up_weight": up_weight, "up_bias": up_bias, "down_weight": down_weight, "ada_weight": ada_weight, "norm_gain": norm_gain, "norm_bias": norm_bias, "out_grad": out_grad}


norm_epsilon = 1e-05
precise = lax.Precision.HIGHEST

@jax.custom_vjp
def low(v):
    return lax.optimization_barrier(v.astype(jnp.bfloat16)).astype(jnp.float32)

@jax.custom_vjp
def low_back(v):
    return v

def low_keep(v):
    return (low(v), None)

def low_pass(kept, grad):
    return (grad,)

def back_keep(v):
    return (v, None)

def back_low(kept, grad):
    return (low(grad),)
low.defvjp(low_keep, low_pass)
low_back.defvjp(back_keep, back_low)

def layer_norm(values):
    center = lax.optimization_barrier(jnp.mean(values, axis=-1, keepdims=True))
    spread = values - center
    second = lax.optimization_barrier(jnp.mean(spread * spread, axis=-1, keepdims=True))
    return spread * lax.rsqrt(second + norm_epsilon)

def rope_tables(length, channels):
    halfway = channels // 2
    freqs = jnp.exp(-math.log(10000.0) * jnp.arange(halfway, dtype=jnp.float32) * (2.0 / channels))
    angle = jnp.arange(length, dtype=jnp.float32)[:, None] * freqs[None, :]
    angle = jnp.concatenate([angle, angle], axis=1)
    return (jnp.cos(angle), jnp.sin(angle))

def time_embed(steps, channels):
    halfway = channels // 2
    freqs = jnp.exp(-math.log(10000.0) * jnp.arange(halfway, dtype=jnp.float32) * (1.0 / halfway))
    angle = steps.astype(jnp.float32)[:, None] * freqs[None, :]
    return jnp.concatenate([jnp.cos(angle), jnp.sin(angle)], axis=1)

def rotate(values, cosine, sine):
    halfway = values.shape[-1] // 2
    turned = jnp.concatenate([-values[..., halfway:], values[..., :halfway]], axis=-1)
    return values * cosine + turned * sine

def attend_packed(packed):
    queries, keys_in, values_in = packed
    scores = low_back(jnp.einsum('qhd,khd->hqk', queries, keys_in, precision=precise) * HD ** (-0.5))
    weights = low(jax.nn.softmax(scores, axis=-1))
    return jnp.einsum('hqk,khd->qhd', weights, values_in, precision=precise)

def forward(in_weight, qkv_weight, out_weight, up_weight, up_bias, down_weight, ada_weight, norm_gain, norm_bias, noisy_in, self_in, flag_rows, embed):
    seq_count = noisy_in.shape[0] // LEN
    cosine, sine = rope_tables(LEN, HD)
    cos_heads = cosine[:, None, :]
    sin_heads = sine[:, None, :]
    joined = jnp.concatenate([noisy_in, self_in * flag_rows[:, None]], axis=1)
    hidden = low_back(jnp.dot(joined, in_weight, precision=precise))
    normed = low(layer_norm(hidden) * norm_gain + norm_bias)

    def heads_of(weight):
        return low_back(jnp.dot(normed, weight, precision=precise)).reshape(seq_count, LEN, H, HD)
    queries = low(rotate(heads_of(qkv_weight[0]), cos_heads, sin_heads))
    keys_in = low(rotate(heads_of(qkv_weight[1]), cos_heads, sin_heads))
    values_in = low(heads_of(qkv_weight[2]))
    mixed = lax.map(jax.checkpoint(attend_packed), (queries, keys_in, values_in))
    mixed = low(low_back(mixed.reshape(seq_count * LEN, D)))
    resid = hidden + low_back(jnp.dot(mixed, out_weight, precision=precise))
    ada = jnp.repeat(jnp.dot(embed, ada_weight, precision=precise), LEN, axis=0)
    modulated = low((1.0 + ada[:, D:2 * D]) * layer_norm(resid) + ada[:, :D])
    pre_act = low_back(jnp.dot(modulated, up_weight, precision=precise) + up_bias)
    activ = low(jax.nn.gelu(pre_act, approximate=False))
    branch = low_back(jnp.dot(activ, down_weight, precision=precise))
    return resid + ada[:, 2 * D:] * branch

def reference(noisy_embed, self_cond, cond_flag, timestep, in_weight, qkv_weight, out_weight, up_weight, up_bias, down_weight, ada_weight, norm_gain, norm_bias, out_grad):
    weights = tuple((item.astype(jnp.float32) for item in (in_weight, qkv_weight, out_weight, up_weight, up_bias, down_weight, ada_weight, norm_gain, norm_bias)))
    blocks = SEQS // SEQ_DEV
    span = SEQ_DEV * LEN
    noisy_all = noisy_embed.astype(jnp.float32).reshape(blocks, span, EMB)
    self_all = self_cond.astype(jnp.float32).reshape(blocks, span, EMB)
    flag_all = cond_flag.reshape(blocks, SEQ_DEV)
    time_all = timestep.reshape(blocks, SEQ_DEV)
    grad_all = out_grad.astype(jnp.float32).reshape(blocks, span, D)

    def step(totals, packed):
        noisy_one, self_one, flag_one, time_one, grad_one = packed
        embed = low(time_embed(time_one, TE))
        flag_rows = jnp.repeat(flag_one.astype(jnp.float32), LEN)

        def run(params, noisy_in, self_in):
            return forward(*params, noisy_in, self_in, flag_rows, embed)
        output, pull = jax.vjp(run, weights, noisy_one, self_one)
        grad_params, grad_noisy, grad_self = pull(grad_one)
        totals = tuple((old + new for old, new in zip(totals, grad_params)))
        return (totals, (output, grad_noisy, grad_self))
    zeros = tuple((jnp.zeros_like(item) for item in weights))
    sums, (outputs, grad_noisy, grad_self) = lax.scan(step, zeros, (noisy_all, self_all, flag_all, time_all, grad_all))
    return (outputs.reshape(SEQS * LEN, D), grad_noisy.reshape(SEQS * LEN, EMB), grad_self.reshape(SEQS * LEN, EMB), sums[0], sums[1], sums[2], sums[3], sums[4], sums[5], sums[6], sums[7], sums[8])
```

```python
import functools
import math

import jax
import jax.numpy as jnp
import numpy as np
from jax import lax
from jax.experimental import pallas as pl
from jax.experimental.pallas import tpu as pltpu
from jax.sharding import PartitionSpec as P

HD = 64
SPLIT = 8
norm_epsilon = 1e-05
precise = lax.Precision.HIGHEST
f32, bf16 = jnp.float32, jnp.bfloat16


def nt(left, right):
    return lax.dot_general(left, right, (((1,), (1,)), ((), ())), preferred_element_type=f32)


def nn(left, right):
    return lax.dot_general(left, right, (((1,), (0,)), ((), ())), preferred_element_type=f32)


def tn(left, right):
    return lax.dot_general(left, right, (((0,), (0,)), ((), ())), preferred_element_type=f32)


def swap_halves(values):
    width = values.shape[1]
    lane = lax.broadcasted_iota(jnp.int32, values.shape, 1)
    return jnp.where(
        lane % HD < HD // 2,
        pltpu.roll(values, width - HD // 2, 1),
        pltpu.roll(values, HD // 2, 1),
    )


def attend_kernel(
    rows_own, x_ref, wq_ref, wk_ref, wv_ref, cos_ref, sin_ref, q_ref, k_ref, v_ref, m_ref, mf_ref, l_ref
):
    wide = wq_ref.shape[1]
    reps = wide // 128
    cosine = jnp.concatenate([cos_ref[...]] * reps, axis=1)
    sine = jnp.concatenate([sin_ref[...]] * reps, axis=1)
    proj = nt(x_ref[:rows_own, :], wq_ref[0])
    proj = proj * cosine[:rows_own] + swap_halves(proj) * sine[:rows_own]
    q_ref[...] = (proj * HD**-0.5).astype(bf16)
    proj = nt(x_ref[...], wk_ref[0])
    k_ref[...] = (proj * cosine + swap_halves(proj) * sine).astype(bf16)
    v_ref[...] = nt(x_ref[...], wv_ref[0]).astype(bf16)
    lane = lax.broadcasted_iota(jnp.int32, (rows_own, 128), 1)
    for pair in range(reps):
        cols = pl.ds(pair * 128, 128)
        keys, values, queries = k_ref[:, cols], v_ref[:, cols], q_ref[:, cols]
        out = stat = None
        for head in range(2):
            scores = nt(jnp.where(lane // HD == head, queries, jnp.zeros_like(queries)), keys)
            top = jnp.max(scores, axis=1, keepdims=True)
            probs = jnp.exp(scores - top)
            total = jnp.sum(probs, axis=1, keepdims=True)
            mixed = nn(probs.astype(bf16), values) * (1.0 / total)
            log_total = jnp.broadcast_to(top + jnp.log(total), (rows_own, 128))
            out = mixed if head == 0 else jnp.where(lane < HD, out, mixed)
            stat = log_total if head == 0 else jnp.where(lane < HD, stat, log_total)
        m_ref[:, cols] = out.astype(bf16)
        mf_ref[:, cols] = out
        l_ref[:, cols] = stat


def attend(x, weights, cosine, sine, rows_own):
    length, features = x.shape
    wide = 256
    spec = lambda m: pl.BlockSpec((1, wide, features), lambda i: (m, i, 0))
    table = pl.BlockSpec((length, 128), lambda i: (0, 0))
    col = lambda n: pl.BlockSpec((n, wide), lambda i: (0, i))
    shape = lambda n, kind: jax.ShapeDtypeStruct((n, features), kind)
    return pl.pallas_call(
        functools.partial(attend_kernel, rows_own),
        grid=(features // wide,),
        in_specs=[pl.BlockSpec((length, features), lambda i: (0, 0)), spec(0), spec(1), spec(2), table, table],
        out_specs=[col(rows_own), col(length), col(length), col(rows_own), col(rows_own), col(rows_own)],
        out_shape=[
            shape(rows_own, bf16), shape(length, bf16), shape(length, bf16),
            shape(rows_own, bf16), shape(rows_own, f32), shape(rows_own, f32),
        ],
        compiler_params=pltpu.CompilerParams(vmem_limit_bytes=40 << 20),
        cost_estimate=pl.CostEstimate(
            flops=8 * length * features * features + 4 * rows_own * length * features,
            bytes_accessed=14 << 20,
            transcendentals=rows_own * length * features // HD,
        ),
        name="attend_fwd",
    )(x, weights, weights, weights, cosine, sine)


def attend_back_kernel(
    q_ref, k_ref, v_ref, g_ref, mf_ref, l_ref, cos_ref, sin_ref, dq_ref, dk_ref, dv_ref, acc_k, acc_v
):
    keys, values, queries, grads = k_ref[...], v_ref[...], q_ref[...], g_ref[...]
    rows = queries.shape[0]
    lane = lax.broadcasted_iota(jnp.int32, queries.shape, 1)
    product = grads.astype(f32) * mf_ref[...]
    grad_q = None
    for head in range(2):
        mine = lane // HD == head
        q_head = jnp.where(mine, queries, jnp.zeros_like(queries))
        g_head = jnp.where(mine, grads, jnp.zeros_like(grads))
        center = jnp.sum(jnp.where(mine, product, 0.0), axis=1, keepdims=True)
        probs = jnp.exp(nt(q_head, keys) - l_ref[:, pl.ds(head * HD, 1)])
        grad_prob = nt(g_head, values)
        grad_score = (probs * (grad_prob - center)).astype(bf16)
        part = nn(grad_score, keys) * HD**-0.5
        grad_q = part if head == 0 else jnp.where(lane < HD, grad_q, part)
        part_v = tn(probs.astype(bf16), g_head)
        part_k = tn(grad_score, q_head)
        if head == 0:
            acc_k[...] = part_k
            acc_v[...] = part_v
        else:
            dk = acc_k[...] + part_k
            dv = acc_v[...] + part_v
    dq_ref[...] = (grad_q * cos_ref[:rows, :] + swap_halves(grad_q * sin_ref[:rows, :])).astype(bf16)
    dk_ref[...] = (dk * cos_ref[...] + swap_halves(dk * sin_ref[...])).astype(bf16)
    dv_ref[...] = dv.astype(bf16)


def attend_back(q, k, v, grads, mixed, log_total, cosine, sine):
    (rows, features), length, wide = q.shape, k.shape[0], 128
    col = lambda n: pl.BlockSpec((n, wide), lambda i: (0, i))
    table = pl.BlockSpec((length, 128), lambda i: (0, 0))
    shape = lambda n: jax.ShapeDtypeStruct((n, features), bf16)
    return pl.pallas_call(
        attend_back_kernel,
        grid=(features // wide,),
        in_specs=[col(rows), col(length), col(length), col(rows), col(rows), col(rows), table, table],
        out_specs=[col(rows), col(length), col(length)],
        out_shape=[shape(rows), shape(length), shape(length)],
        scratch_shapes=[pltpu.VMEM((length, wide), f32)] * 2,
        compiler_params=pltpu.CompilerParams(vmem_limit_bytes=40 << 20),
        cost_estimate=pl.CostEstimate(
            flops=10 * rows * length * features,
            bytes_accessed=12 << 20,
            transcendentals=rows * length * features // HD,
        ),
        name="attend_bwd",
    )(q, k, v, grads, mixed, log_total, cosine, sine)


def norm_stats(values):
    center = jnp.mean(values, axis=-1, keepdims=True)
    spread = values - center
    second = jnp.mean(spread * spread, axis=-1, keepdims=True)
    inverse = lax.rsqrt(second + norm_epsilon)
    return spread * inverse, inverse


def norm_back(normed, inverse, upstream):
    first = jnp.mean(upstream, axis=-1, keepdims=True)
    cross = jnp.mean(upstream * normed, axis=-1, keepdims=True)
    return (upstream - first - normed * cross) * inverse


def rope_tables(length, first):
    halfway = HD // 2
    freqs = np.exp(-np.float32(math.log(10000.0)) * np.arange(halfway, dtype=np.float32) * np.float32(2.0 / HD))
    angle = np.arange(length, dtype=np.float32)[:, None] * freqs[None, :].astype(np.float32)
    cosine, sine = np.cos(angle), np.sin(angle)
    both = np.concatenate([np.tile(cosine, (1, 4)), np.tile(np.concatenate([-sine, sine], 1), (1, 2))], 1)
    both = jnp.asarray(np.concatenate([both, both], 0).astype(np.float32))
    both = lax.dynamic_slice_in_dim(both, first, length, 0)
    return both[:, :128], both[:, 128:]


def time_embed(steps, channels):
    halfway = channels // 2
    freqs = jnp.exp(-math.log(10000.0) * jnp.arange(halfway, dtype=f32) * (1.0 / halfway))
    angle = steps.astype(f32)[:, None] * freqs[None, :]
    return jnp.concatenate([jnp.cos(angle), jnp.sin(angle)], axis=1)


def gelu_both(values):
    phi = 0.5 * (1.0 + lax.erf(values * math.sqrt(0.5)))
    bell = jnp.exp(-0.5 * values * values) * (1.0 / math.sqrt(2.0 * math.pi))
    return values * phi, phi + values * bell


def pick(array, index, axis=0):
    return lax.dynamic_index_in_dim(array, index, axis, keepdims=False)


class Links:
    def __init__(self):
        self.n_t = lax.axis_size("tensor")
        self.n_dp = lax.axis_size("dp")
        self.tensor = lax.axis_index("tensor")
        self.dp = lax.axis_index("dp")
        self.low = self.dp % SPLIT

    def swap(self, array, dp_bits, tensor_bits):
        pairs = [
            (d * self.n_t + t, (d ^ dp_bits) * self.n_t + (t ^ tensor_bits))
            for d in range(self.n_dp)
            for t in range(self.n_t)
        ]
        return lax.ppermute(array, ("dp", "tensor"), pairs)

    def plane(self, array):
        return [array] + [self.swap(array, 2 * j, 0) for j in range(1, SPLIT // 2)]

    def spread(self, piece):
        far = jnp.stack([self.swap(piece, 0, k) for k in range(1, self.n_t)])
        mine = self.plane(far)
        return [mine, list(self.swap(jnp.stack(mine), 1, 0))]

    def reduce(self, near, other):
        total = near.astype(f32) + self.swap(other, 1, 0).astype(f32)
        total = [total[0]] + [self.swap(total[j].astype(bf16), 2 * j, 0) for j in range(1, SPLIT // 2)]
        total = sum(t.astype(f32) for t in total)
        total = [total[0]] + [self.swap(total[k].astype(bf16), 0, k) for k in range(1, self.n_t)]
        total = sum(t.astype(f32) for t in total)
        bit = SPLIT
        while bit < self.n_dp:
            total = total + self.swap(total, bit, 0)
            bit *= 2
        return total

    def collect(self, piece):
        mine = jnp.stack(self.plane(piece.astype(bf16)))
        both = jnp.stack([mine, self.swap(mine, 1, 0)], axis=1)
        both = both.reshape((SPLIT,) + piece.shape)
        return jnp.stack([pick(both, self.low ^ a) for a in range(SPLIT)])

    def add_all(self, array):
        bit = 1
        while bit < self.n_t:
            array = array + self.swap(array, 0, bit)
            bit *= 2
        bit = 1
        while bit < self.n_dp:
            array = array + self.swap(array, bit, 0)
            bit *= 2
        return array

    def gather_all(self, array):
        bit = 1
        while bit < self.n_t:
            array = jnp.concatenate([array, self.swap(array, 0, bit)])
            bit *= 2
        bit = 1
        while bit < self.n_dp:
            array = jnp.concatenate([array, self.swap(array, bit, 0)])
            bit *= 2
        return array


def on_device(
    noisy_embed, self_cond, cond_flag, timestep, in_weight, qkv_weight, out_weight,
    up_weight, up_bias, down_weight, ada_weight, norm_gain, norm_bias, out_grad,
):
    links = Links()
    n_t, low = links.n_t, links.low
    rows, features = out_grad.shape
    embed_cols = noisy_embed.shape[1]
    seq_len = rows * n_t // cond_flag.shape[0]
    assert seq_len == 2 * rows
    head_cols = qkv_weight.shape[2]
    hidden_cols = up_weight.shape[1]
    kinds = 4

    attn_quarter = jnp.stack(
        [qkv_weight[0].T, qkv_weight[1].T, qkv_weight[2].T, out_weight]
    ).reshape(kinds, SPLIT, head_cols // SPLIT, features)
    attn_far = links.spread(pick(attn_quarter, low, 1))
    rel = jnp.stack([jnp.stack(attn_far[i]) if i == 0 else jnp.stack(attn_far[i]) for i in range(2)], axis=1)
    rel = rel.reshape((SPLIT,) + rel.shape[2:])
    far = jnp.stack([pick(rel, low ^ a) for a in range(SPLIT)], axis=2)
    far = jnp.moveaxis(far.reshape(n_t - 1, kinds, head_cols, features), 0, 1)
    attn_weights = jnp.concatenate(
        [attn_quarter.reshape(kinds, 1, head_cols, features), far], axis=1
    ).reshape(kinds, n_t * head_cols, features)

    part_cols = hidden_cols // SPLIT
    ff_quarter = jnp.stack(
        [up_weight.T.reshape(SPLIT, part_cols, features), down_weight.reshape(SPLIT, part_cols, features)], axis=1
    )
    ff_far = links.spread(pick(ff_quarter, low))
    bias_quarters = [up_bias] + [links.swap(up_bias, 0, k) for k in range(1, n_t)]
    bias_all = jnp.stack(bias_quarters).reshape(n_t, SPLIT, part_cols).astype(f32)
    ups, downs, biases = [], [], []
    for i in range(2):
        up_list, down_list, bias_list = [], [], []
        for j in range(SPLIT // 2):
            where = low ^ (j * 2 + i)
            here = pick(ff_quarter, where)
            up_list += [here[0]] + [ff_far[i][j][k, 0] for k in range(n_t - 1)]
            down_list += [here[1]] + [ff_far[i][j][k, 1] for k in range(n_t - 1)]
            bias_list.append(pick(bias_all, where, 1))
        ups.append(jnp.concatenate(up_list))
        downs.append(jnp.concatenate(down_list))
        biases.append(jnp.concatenate(bias_list).reshape(1, -1))

    sequence = (links.tensor * rows) // seq_len
    flag = pick(cond_flag, sequence).astype(f32)
    embed_low = time_embed(lax.dynamic_slice_in_dim(timestep, sequence, 1, 0), ada_weight.shape[0]).astype(bf16)
    ada = jnp.dot(embed_low, ada_weight, preferred_element_type=f32)
    shift, scale, gate = ada[:, :features], 1.0 + ada[:, features : 2 * features], ada[:, 2 * features :]

    joined = jnp.concatenate([noisy_embed, (self_cond.astype(f32) * flag).astype(bf16)], axis=1)
    joined = jnp.concatenate([joined, links.swap(joined, 0, 1)])
    cosine, sine = rope_tables(seq_len, (links.tensor * rows) % seq_len)
    hidden = jnp.dot(joined, in_weight, preferred_element_type=f32)
    normed_one, inverse_one = norm_stats(hidden)
    attn_in = (normed_one * norm_gain + norm_bias).astype(bf16)
    q, k, v, mixed, mixed_full, log_total = attend(attn_in, attn_weights, cosine, sine, rows)
    resid = hidden[:rows] + nn(mixed, attn_weights[3])
    normed_two, inverse_two = norm_stats(resid)
    modulated = (scale * normed_two + shift).astype(bf16)
    acts, slopes, branch = [], [], 0.0
    for i in range(2):
        act, slope = gelu_both(nt(modulated, ups[i]) + biases[i])
        acts.append(act.astype(bf16))
        slopes.append(slope.astype(bf16))
        branch = branch + nn(acts[i], downs[i])
    result = resid + gate * branch

    grad_branch = (gate * out_grad).astype(bf16)
    grad_ups, grad_downs, grad_biases, grad_mod = [], [], [], 0.0
    for i in range(2):
        grad_downs.append(tn(acts[i], grad_branch).astype(bf16))
        grad_pre = (slopes[i].astype(f32) * nt(grad_branch, downs[i])).astype(bf16)
        grad_biases.append(jnp.sum(grad_pre.astype(f32), axis=0))
        grad_ups.append(tn(grad_pre, modulated).astype(bf16))
        grad_mod = grad_mod + nn(grad_pre, ups[i])
    ff_shape = (SPLIT // 2, n_t, part_cols, features)
    down_piece = links.reduce(grad_downs[0].reshape(ff_shape), grad_downs[1].reshape(ff_shape))
    up_piece = links.reduce(grad_ups[0].reshape(ff_shape), grad_ups[1].reshape(ff_shape))
    grad_down = links.collect(down_piece).reshape(hidden_cols, features).astype(f32)
    grad_up = links.collect(up_piece).reshape(hidden_cols, features).T.astype(f32)

    grad_resid = out_grad + norm_back(normed_two, inverse_two, scale * grad_mod)
    grad_ada_row = jnp.concatenate(
        [
            jnp.sum(grad_mod, axis=0),
            jnp.sum(grad_mod * normed_two, axis=0),
            jnp.sum(out_grad * branch, axis=0),
            embed_low[0].astype(f32),
        ]
    )[None]
    ada_rows = links.gather_all(grad_ada_row)
    grad_ada = lax.dot_general(
        ada_rows[:, 3 * features :], ada_rows[:, : 3 * features],
        (((0,), (0,)), ((), ())), precision=precise, preferred_element_type=f32,
    )

    grad_attn = grad_resid.astype(bf16)
    grad_out_w = tn(mixed, grad_attn).astype(bf16)
    grad_mixed = nt(grad_attn, attn_weights[3]).astype(bf16)
    grad_q, grad_k, grad_v = attend_back(q, k, v, grad_mixed, mixed_full, log_total, cosine, sine)
    grad_q_w = tn(grad_q, attn_in[:rows]).astype(bf16)
    grad_k_w = tn(grad_k, attn_in).astype(bf16)
    grad_v_w = tn(grad_v, attn_in).astype(bf16)
    core = low % 2
    sides = low // 2

    def reduce_attn(grads):
        parts = jnp.stack(grads).reshape(len(grads), n_t, SPLIT // 2, 2, head_cols // SPLIT, features)
        near = jnp.stack([pick(pick(parts, core, 3), sides ^ j, 2) for j in range(SPLIT // 2)])
        other = jnp.stack([pick(pick(parts, 1 - core, 3), sides ^ j, 2) for j in range(SPLIT // 2)])
        piece = links.reduce(jnp.moveaxis(near, 2, 1), jnp.moveaxis(other, 2, 1))
        full = links.collect(piece)
        return jnp.moveaxis(full, 0, 1).reshape(len(grads), head_cols, features).astype(f32)

    grad_out = reduce_attn([grad_out_w])[0]
    grad_qkv = jnp.swapaxes(reduce_attn([grad_q_w, grad_k_w, grad_v_w]), 1, 2)

    grad_norm = nn(grad_k, attn_weights[1]) + nn(grad_v, attn_weights[2])
    grad_norm = jnp.concatenate([grad_norm[:rows] + nn(grad_q, attn_weights[0]), grad_norm[rows:]])
    grad_gain = jnp.sum(grad_norm * normed_one, axis=0)
    grad_offset = jnp.sum(grad_norm, axis=0)
    grad_hidden = norm_back(normed_one, inverse_one, grad_norm * norm_gain)
    grad_hidden = jnp.concatenate([grad_hidden[:rows] + grad_resid, grad_hidden[rows:]]).astype(bf16)
    grad_in = tn(joined, grad_hidden)
    grad_joined = nt(grad_hidden, in_weight)
    grad_joined = grad_joined[:rows] + links.swap(grad_joined[rows:], 0, 1)
    grad_noisy = grad_joined[:, :embed_cols]
    grad_self = grad_joined[:, embed_cols:] * flag

    bias_rel = jnp.stack([b.reshape(SPLIT // 2, n_t, part_cols) for b in grad_biases], axis=1)
    bias_rel = bias_rel.reshape(SPLIT, n_t, part_cols)
    bias_abs = jnp.stack([pick(bias_rel, low ^ a) for a in range(SPLIT)], axis=1).reshape(n_t, hidden_cols)
    bias_abs = jnp.stack([pick(bias_abs, links.tensor ^ t) for t in range(n_t)])
    bias_pad = jnp.reshape(bias_abs, (-1, features))
    small = links.add_all(jnp.concatenate([grad_in, grad_gain[None], grad_offset[None], bias_pad]))
    n_in = grad_in.shape[0]
    grad_in, grad_gain, grad_offset = small[:n_in], small[n_in], small[n_in + 1]
    grad_bias = pick(small[n_in + 2 :].reshape(n_t, hidden_cols), links.tensor)
    return (
        result, grad_noisy, grad_self, grad_in, grad_qkv, grad_out, grad_up,
        grad_bias, grad_down, grad_ada, grad_gain, grad_offset,
    )


def solution(mesh):
    tokens = P(("dp", "tensor"), None)
    return jax.shard_map(
        on_device,
        mesh=mesh,
        in_specs=(
            tokens, tokens, P("dp"), P("dp"), P(), P(None, None, "tensor"), P("tensor", None),
            P(None, "tensor"), P("tensor"), P("tensor", None), P(), P(), P(), tokens,
        ),
        out_specs=(
            tokens, tokens, tokens, P(), P(None, None, "tensor"), P("tensor", None), P(None, "tensor"),
            P("tensor"), P("tensor", None), P(), P(), P(),
        ),
        check_vma=False,
    )
```

```python
import functools
import math

import jax
import jax.numpy as jnp
import numpy as np
from jax import lax
from jax.experimental import pallas as pl
from jax.experimental.pallas import tpu as pltpu
from jax.sharding import PartitionSpec as P

HD = 64
SPLIT = 8
norm_epsilon = 1e-05
precise = lax.Precision.HIGHEST
f32, bf16 = jnp.float32, jnp.bfloat16
MESH = pl.DeviceIdType.MESH


def nt(left, right):
    return lax.dot_general(left, right, (((1,), (1,)), ((), ())), preferred_element_type=f32)


def nn(left, right):
    return lax.dot_general(left, right, (((1,), (0,)), ((), ())), preferred_element_type=f32)


def tn(left, right):
    return lax.dot_general(left, right, (((0,), (0,)), ((), ())), preferred_element_type=f32)


def swap_halves(values):
    width = values.shape[1]
    lane = lax.broadcasted_iota(jnp.int32, values.shape, 1)
    return jnp.where(
        lane % HD < HD // 2,
        pltpu.roll(values, width - HD // 2, 1),
        pltpu.roll(values, HD // 2, 1),
    )


def attend_kernel(
    rows_own, x_ref, wq_ref, wk_ref, wv_ref, cos_ref, sin_ref, q_ref, k_ref, v_ref, m_ref, mf_ref, l_ref
):
    wide = wq_ref.shape[0] * wq_ref.shape[2]
    reps = wide // 128
    cosine = jnp.concatenate([cos_ref[...]] * reps, axis=1)
    sine = jnp.concatenate([sin_ref[...]] * reps, axis=1)
    proj = nt(x_ref[:rows_own, :], wq_ref[...].reshape(wide, -1))
    proj = proj * cosine[:rows_own] + swap_halves(proj) * sine[:rows_own]
    q_ref[...] = (proj * HD**-0.5).astype(bf16)
    proj = nt(x_ref[...], wk_ref[...].reshape(wide, -1))
    k_ref[...] = (proj * cosine + swap_halves(proj) * sine).astype(bf16)
    v_ref[...] = nt(x_ref[...], wv_ref[...].reshape(wide, -1)).astype(bf16)
    lane = lax.broadcasted_iota(jnp.int32, (rows_own, 128), 1)
    for pair in range(reps):
        cols = pl.ds(pair * 128, 128)
        keys, values, queries = k_ref[:, cols], v_ref[:, cols], q_ref[:, cols]
        out = stat = None
        for head in range(2):
            scores = nt(jnp.where(lane // HD == head, queries, jnp.zeros_like(queries)), keys)
            top = jnp.max(scores, axis=1, keepdims=True)
            probs = jnp.exp(scores - top)
            total = jnp.sum(probs, axis=1, keepdims=True)
            mixed = nn(probs.astype(bf16), values) * (1.0 / total)
            log_total = jnp.broadcast_to(top + jnp.log(total), (rows_own, 128))
            out = mixed if head == 0 else jnp.where(lane < HD, out, mixed)
            stat = log_total if head == 0 else jnp.where(lane < HD, stat, log_total)
        m_ref[:, cols] = out.astype(bf16)
        mf_ref[:, cols] = out
        l_ref[:, cols] = stat


def attend(x, weights, cosine, sine, rows_own):
    length, features = x.shape
    wide = 2 * weights.shape[2]
    spec = lambda m: pl.BlockSpec((2, 1, weights.shape[2], features), lambda i: (i, m, 0, 0))
    table = pl.BlockSpec((length, 128), lambda i: (0, 0))
    col = lambda n: pl.BlockSpec((n, wide), lambda i: (0, i))
    shape = lambda n, kind: jax.ShapeDtypeStruct((n, features), kind)
    return pl.pallas_call(
        functools.partial(attend_kernel, rows_own),
        grid=(features // wide,),
        in_specs=[pl.BlockSpec((length, features), lambda i: (0, 0)), spec(0), spec(1), spec(2), table, table],
        out_specs=[col(rows_own), col(length), col(length), col(rows_own), col(rows_own), col(rows_own)],
        out_shape=[
            shape(rows_own, bf16), shape(length, bf16), shape(length, bf16),
            shape(rows_own, bf16), shape(rows_own, f32), shape(rows_own, f32),
        ],
        compiler_params=pltpu.CompilerParams(vmem_limit_bytes=40 << 20),
        cost_estimate=pl.CostEstimate(
            flops=8 * length * features * features + 4 * rows_own * length * features,
            bytes_accessed=14 << 20,
            transcendentals=rows_own * length * features // HD,
        ),
        name="attend_fwd",
    )(x, weights, weights, weights, cosine, sine)


def attend_back_kernel(
    q_ref, k_ref, v_ref, g_ref, mf_ref, l_ref, cos_ref, sin_ref, dq_ref, dk_ref, dv_ref, acc_k, acc_v
):
    keys, values, queries, grads = k_ref[...], v_ref[...], q_ref[...], g_ref[...]
    rows = queries.shape[0]
    lane = lax.broadcasted_iota(jnp.int32, queries.shape, 1)
    product = grads.astype(f32) * mf_ref[...]
    grad_q = None
    for head in range(2):
        mine = lane // HD == head
        q_head = jnp.where(mine, queries, jnp.zeros_like(queries))
        g_head = jnp.where(mine, grads, jnp.zeros_like(grads))
        center = jnp.sum(jnp.where(mine, product, 0.0), axis=1, keepdims=True)
        probs = jnp.exp(nt(q_head, keys) - l_ref[:, pl.ds(head * HD, 1)])
        grad_prob = nt(g_head, values)
        grad_score = (probs * (grad_prob - center)).astype(bf16)
        part = nn(grad_score, keys) * HD**-0.5
        grad_q = part if head == 0 else jnp.where(lane < HD, grad_q, part)
        part_v = tn(probs.astype(bf16), g_head)
        part_k = tn(grad_score, q_head)
        if head == 0:
            acc_k[...] = part_k
            acc_v[...] = part_v
        else:
            dk = acc_k[...] + part_k
            dv = acc_v[...] + part_v
    dq_ref[...] = (grad_q * cos_ref[:rows, :] + swap_halves(grad_q * sin_ref[:rows, :])).astype(bf16)
    dk_ref[...] = (dk * cos_ref[...] + swap_halves(dk * sin_ref[...])).astype(bf16)
    dv_ref[...] = dv.astype(bf16)


def attend_back(q, k, v, grads, mixed, log_total, cosine, sine):
    (rows, features), length, wide = q.shape, k.shape[0], 128
    col = lambda n: pl.BlockSpec((n, wide), lambda i: (0, i))
    table = pl.BlockSpec((length, 128), lambda i: (0, 0))
    shape = lambda n: jax.ShapeDtypeStruct((n, features), bf16)
    return pl.pallas_call(
        attend_back_kernel,
        grid=(features // wide,),
        in_specs=[col(rows), col(length), col(length), col(rows), col(rows), col(rows), table, table],
        out_specs=[col(rows), col(length), col(length)],
        out_shape=[shape(rows), shape(length), shape(length)],
        scratch_shapes=[pltpu.VMEM((length, wide), f32)] * 2,
        compiler_params=pltpu.CompilerParams(vmem_limit_bytes=40 << 20),
        cost_estimate=pl.CostEstimate(
            flops=10 * rows * length * features,
            bytes_accessed=12 << 20,
            transcendentals=rows * length * features // HD,
        ),
        name="attend_bwd",
    )(q, k, v, grads, mixed, log_total, cosine, sine)


def norm_stats(values):
    center = jnp.mean(values, axis=-1, keepdims=True)
    spread = values - center
    second = jnp.mean(spread * spread, axis=-1, keepdims=True)
    inverse = lax.rsqrt(second + norm_epsilon)
    return spread * inverse, inverse


def norm_back(normed, inverse, upstream):
    first = jnp.mean(upstream, axis=-1, keepdims=True)
    cross = jnp.mean(upstream * normed, axis=-1, keepdims=True)
    return (upstream - first - normed * cross) * inverse


def rope_tables(length, first):
    halfway = HD // 2
    freqs = np.exp(-np.float32(math.log(10000.0)) * np.arange(halfway, dtype=np.float32) * np.float32(2.0 / HD))
    angle = np.arange(length, dtype=np.float32)[:, None] * freqs[None, :].astype(np.float32)
    cosine, sine = np.cos(angle), np.sin(angle)
    both = np.concatenate([np.tile(cosine, (1, 4)), np.tile(np.concatenate([-sine, sine], 1), (1, 2))], 1)
    both = jnp.asarray(np.concatenate([both, both], 0).astype(np.float32))
    both = lax.dynamic_slice_in_dim(both, first, length, 0)
    return both[:, :128], both[:, 128:]


def time_embed(steps, channels):
    halfway = channels // 2
    freqs = jnp.exp(-math.log(10000.0) * jnp.arange(halfway, dtype=f32) * (1.0 / halfway))
    angle = steps.astype(f32)[:, None] * freqs[None, :]
    return jnp.concatenate([jnp.cos(angle), jnp.sin(angle)], axis=1)


def gelu_both(values):
    phi = 0.5 * (1.0 + lax.erf(values * math.sqrt(0.5)))
    bell = jnp.exp(-0.5 * values * values) * (1.0 / math.sqrt(2.0 * math.pi))
    return values * phi, phi + values * bell


def pick(array, index, axis=0):
    return lax.dynamic_index_in_dim(array, index, axis, keepdims=False)


def flip(index, bits):
    bit = 1
    while bit <= bits:
        if bits & bit:
            index = index + bit - 2 * bit * ((index // bit) % 2)
        bit *= 2
    return index


class Net:
    def __init__(self, n_dp, n_t, send_sems, recv_sems):
        self.dp, self.tensor = lax.axis_index("dp"), lax.axis_index("tensor")
        self.low = self.dp % SPLIT
        self.core, self.x, self.y = self.low % 2, (self.low // 2) % 2, self.low // 4
        self.n_t, self.high_bits = n_t, []
        while SPLIT << len(self.high_bits) < n_dp:
            self.high_bits.append(SPLIT << len(self.high_bits))
        self.sems, self.used, self.open = (send_sems, recv_sems), 0, []

    def peers(self):
        return [(b, 0) for b in [1, 2, 4] + self.high_bits] + [(0, k) for k in range(1, self.n_t)]

    def peer(self, bits):
        return {"dp": flip(self.dp, bits[0]), "tensor": flip(self.tensor, bits[1])}

    def barrier(self):
        ready = pltpu.get_barrier_semaphore()
        for bits in self.peers():
            pl.semaphore_signal(ready, inc=1, device_id=self.peer(bits), device_id_type=MESH)
        pl.semaphore_wait(ready, len(self.peers()))

    def send(self, source, target, bits):
        copy = pltpu.make_async_remote_copy(
            src_ref=source, dst_ref=target,
            send_sem=self.sems[0].at[self.used], recv_sem=self.sems[1].at[self.used],
            device_id=self.peer(bits), device_id_type=MESH,
        )
        self.used += 1
        copy.start()
        self.open.append(copy)
        return copy

    def local(self, source, target):
        copy = pltpu.make_async_copy(source, target, self.sems[0].at[self.used])
        self.used += 1
        copy.start()
        return copy

    def close(self):
        for copy in self.open:
            copy.wait_send()
        self.open = []


def rows_of(piece, rows):
    return pl.ds(pl.multiple_of(piece * rows, rows), rows)


def gather_steps(net, quarter, full):
    rows, half = quarter.shape[0] // SPLIT, quarter.shape[1] // 2
    low, far, state = net.low, pl.ds(1, net.n_t - 1), {}
    cols = (pl.ds(0, half), pl.ds(half, half))

    def start():
        mine = rows_of(low, rows)
        state["z"] = [net.send(quarter.at[mine], full.at[k, mine], (0, k)) for k in range(1, net.n_t)]
        state["own"] = net.local(quarter, full.at[0])

    def plane():
        for copy in state["z"]:
            copy.wait_recv()
        mine = full.at[far, rows_of(low, rows)]
        state["x"], state["y"] = net.send(mine, mine, (2, 0)), net.send(mine, mine, (4, 0))
        state["c"] = [net.send(mine, mine, (1, 0))]

    def relay():
        from_x, from_y = rows_of(flip(low, 2), rows), rows_of(flip(low, 4), rows)
        state["x"].wait_recv()
        part = full.at[far, from_x, cols[0]]
        state["rx"] = net.send(part, part, (4, 0))
        whole = full.at[far, from_x]
        state["c"].append(net.send(whole, whole, (1, 0)))
        state["y"].wait_recv()
        part = full.at[far, from_y, cols[1]]
        state["ry"] = net.send(part, part, (2, 0))
        whole = full.at[far, from_y]
        state["c"].append(net.send(whole, whole, (1, 0)))

    def across():
        state["rx"].wait_recv()
        state["ry"].wait_recv()
        whole = full.at[far, rows_of(flip(low, 6), rows)]
        state["c"].append(net.send(whole, whole, (1, 0)))

    def finish():
        for copy in state["c"]:
            copy.wait_recv()
        state["own"].wait()

    return [start, plane, relay, across, finish]


def collect_steps(net, out):
    half, low, state = out.shape[2] // 2, net.low, {}
    cols = (pl.ds(0, half), pl.ds(half, half))

    def start():
        mine = out.at[low]
        state["x"], state["y"] = net.send(mine, mine, (2, 0)), net.send(mine, mine, (4, 0))
        state["c"] = [net.send(mine, mine, (1, 0))]

    def relay():
        from_x, from_y = flip(low, 2), flip(low, 4)
        state["x"].wait_recv()
        part = out.at[from_x, :, cols[0]]
        state["rx"] = net.send(part, part, (4, 0))
        state["c"].append(net.send(out.at[from_x], out.at[from_x], (1, 0)))
        state["y"].wait_recv()
        part = out.at[from_y, :, cols[1]]
        state["ry"] = net.send(part, part, (2, 0))
        state["c"].append(net.send(out.at[from_y], out.at[from_y], (1, 0)))

    def across():
        state["rx"].wait_recv()
        state["ry"].wait_recv()
        diagonal = out.at[flip(low, 6)]
        state["c"].append(net.send(diagonal, diagonal, (1, 0)))

    def finish():
        for copy in state["c"]:
            copy.wait_recv()

    return [start, relay, across, finish]


def reduce_buffers(n_t, rows, cols, n_high):
    half = cols // 2
    kinds = [
        (n_t, 2, 2, rows, cols), (n_t, 2, 2, rows, cols), (n_t, 2, rows, half), (n_t, 2, rows, half),
        (n_t, rows, half), (n_t, rows, half), (n_t, rows, cols), (n_t, rows, cols), (n_high + 1, rows, cols),
    ]
    return [pltpu.VMEM(shape, bf16) for shape in kinds]


def reduce_steps(net, sources, buffers, out):
    own, came, by_x, by_y, then_y, then_x, summed, away, more = buffers
    half, state = own.shape[4] // 2, {}
    first, second = pl.ds(0, half), pl.ds(half, half)
    n_t, x, y = net.n_t, net.x, net.y

    def start():
        state["own"] = [net.local(view, place(own)) for view, place in sources(net.core)]
        state["c"] = [net.send(view, place(came), (1, 0)) for view, place in sources(1 - net.core)]

    def add_core():
        for copy in state["own"]:
            copy.wait()
        for copy in state["c"]:
            copy.wait_recv()

        def add(i, carry):
            k, j = i // 4, i % 4
            total = own[k, j // 2, j % 2].astype(f32) + came[k, j // 2, j % 2].astype(f32)
            own[k, j // 2, j % 2] = total.astype(bf16)
            return carry

        lax.fori_loop(0, 4 * n_t, add, 0)
        state["x"] = net.send(own.at[:, :, 1 - x, :, first], by_x, (2, 0))
        state["y"] = net.send(own.at[:, 1 - y, :, :, second], by_y, (4, 0))

    def add_first():
        state["x"].wait_recv()
        state["y"].wait_recv()

        def add(i, carry):
            k, j = i // 2, i % 2
            by_x[k, j] = (own[k, j, x, :, first].astype(f32) + by_x[k, j].astype(f32)).astype(bf16)
            by_y[k, j] = (own[k, y, j, :, second].astype(f32) + by_y[k, j].astype(f32)).astype(bf16)
            return carry

        lax.fori_loop(0, 2 * n_t, add, 0)
        state["xy"] = net.send(by_x.at[:, 1 - y], then_y, (4, 0))
        state["yx"] = net.send(by_y.at[:, 1 - x], then_x, (2, 0))

    def add_second():
        state["xy"].wait_recv()
        state["yx"].wait_recv()

        def add(k, carry):
            summed[k, :, first] = (by_x[k, y].astype(f32) + then_y[k].astype(f32)).astype(bf16)
            summed[k, :, second] = (by_y[k, x].astype(f32) + then_x[k].astype(f32)).astype(bf16)
            return carry

        lax.fori_loop(0, n_t, add, 0)
        state["z"] = [net.send(summed.at[k], away.at[k], (0, k)) for k in range(1, n_t)]

    def add_tensor():
        for copy in state["z"]:
            copy.wait_recv()
        total = summed[0].astype(f32)
        for k in range(1, n_t):
            total = total + away[k].astype(f32)
        for n, bit in enumerate(net.high_bits):
            more[0] = total.astype(bf16)
            copy = net.send(more.at[0], more.at[n + 1], (bit, 0))
            net.open.pop()
            copy.wait_recv()
            copy.wait_send()
            total = total + more[n + 1].astype(f32)
        out[net.low] = total.astype(bf16)

    return [start, add_core, add_first, add_second, add_tensor] + collect_steps(net, out)


ANY = pl.BlockSpec(memory_space=pl.ANY)
VMEM = pl.BlockSpec(memory_space=pltpu.VMEM)


def gather_kernel(
    n_dp, n_t, joined_ref, bias_ref, a_ref, u_ref, d_ref,
    joined_out, bias_out, a_out, u_out, d_out, send_sems, recv_sems,
):
    net = Net(n_dp, n_t, send_sems, recv_sems)
    net.barrier()
    small = [net.send(joined_ref, joined_out, (0, 1))]
    small += [net.send(bias_ref, bias_out.at[k], (0, k)) for k in range(1, n_t)]
    bias_out[0] = bias_ref[...]
    a, u, d = gather_steps(net, a_ref, a_out), gather_steps(net, u_ref, u_out), gather_steps(net, d_ref, d_out)
    for group, step in (
        (a, 0), (a, 1), (u, 0), (a, 2), (u, 1), (d, 0), (a, 3), (u, 2), (d, 1), (u, 3), (d, 2), (d, 3),
        (a, 4), (u, 4), (d, 4),
    ):
        group[step]()
    for copy in small:
        copy.wait_recv()
    net.close()


def gather(joined, bias, quarters):
    n_dp, n_t = lax.axis_size("dp"), lax.axis_size("tensor")
    full = [jax.ShapeDtypeStruct((n_t,) + w.shape, bf16) for w in quarters]
    return pl.pallas_call(
        functools.partial(gather_kernel, n_dp, n_t),
        in_specs=[VMEM] * (2 + len(quarters)),
        out_specs=[VMEM, VMEM] + [ANY] * len(quarters),
        out_shape=[
            jax.ShapeDtypeStruct(joined.shape, joined.dtype),
            jax.ShapeDtypeStruct((n_t,) + bias.shape, bias.dtype),
        ] + full,
        scratch_shapes=[pltpu.SemaphoreType.DMA((64,))] * 2,
        compiler_params=pltpu.CompilerParams(collective_id=0, has_side_effects=True, vmem_limit_bytes=40 << 20),
        name="gather_weights",
    )(joined, bias, *quarters)


def reduce_kernel(n_dp, n_t, d_ref, u_ref, q_ref, k_ref, v_ref, o_ref, d_out, u_out, a_out, *scratch):
    send_sems, recv_sems = scratch[-2:]
    net = Net(n_dp, n_t, send_sems, recv_sems)
    net.barrier()
    whole = lambda ref: lambda side: [(ref.at[:, :, :, side], lambda b: b)]
    kinds = (q_ref, k_ref, v_ref, o_ref)
    by_kind = lambda side: [
        (ref.at[:, side], lambda b, m=m: b.at[:, m // 2, m % 2]) for m, ref in enumerate(kinds)
    ]
    count = (len(scratch) - 2) // 3
    d = reduce_steps(net, whole(d_ref), scratch[:count], d_out)
    u = reduce_steps(net, whole(u_ref), scratch[count : 2 * count], u_out)
    a = reduce_steps(net, by_kind, scratch[2 * count : 3 * count], a_out)
    for turn in range(len(d) + 2):
        for lag, group in enumerate((d, u, a)):
            if 0 <= turn - lag < len(group):
                group[turn - lag]()
    net.close()


def reduce_all(grad_down, grad_up, grad_kinds):
    n_dp, n_t = lax.axis_size("dp"), lax.axis_size("tensor")
    rows, cols = grad_down.shape[1] // SPLIT, grad_down.shape[2]
    n_high = (n_dp // SPLIT).bit_length() - 1
    whole = lambda g: g.reshape(n_t, 2, 2, 2, rows, cols)
    kinds = [g.reshape(n_t, 2, rows, cols) for g in grad_kinds]
    return pl.pallas_call(
        functools.partial(reduce_kernel, n_dp, n_t),
        in_specs=[ANY] * 6,
        out_specs=[VMEM] * 3,
        out_shape=[jax.ShapeDtypeStruct((SPLIT, rows, cols), bf16)] * 3,
        scratch_shapes=reduce_buffers(n_t, rows, cols, n_high) * 3 + [pltpu.SemaphoreType.DMA((96,))] * 2,
        compiler_params=pltpu.CompilerParams(collective_id=1, has_side_effects=True, vmem_limit_bytes=56 << 20),
        name="reduce_grads",
    )(whole(grad_down), whole(grad_up), *kinds)


class Links:
    def __init__(self):
        self.n_t = lax.axis_size("tensor")
        self.n_dp = lax.axis_size("dp")
        self.tensor = lax.axis_index("tensor")
        self.dp = lax.axis_index("dp")
        self.low = self.dp % SPLIT

    def swap(self, array, dp_bits, tensor_bits):
        pairs = [
            (d * self.n_t + t, (d ^ dp_bits) * self.n_t + (t ^ tensor_bits))
            for d in range(self.n_dp)
            for t in range(self.n_t)
        ]
        return lax.ppermute(array, ("dp", "tensor"), pairs)

    def add_all(self, array):
        bit = 1
        while bit < self.n_t:
            array = array + self.swap(array, 0, bit)
            bit *= 2
        bit = 1
        while bit < self.n_dp:
            array = array + self.swap(array, bit, 0)
            bit *= 2
        return array

    def gather_all(self, array):
        bit = 1
        while bit < self.n_t:
            array = jnp.concatenate([array, self.swap(array, 0, bit)])
            bit *= 2
        bit = 1
        while bit < self.n_dp:
            array = jnp.concatenate([array, self.swap(array, bit, 0)])
            bit *= 2
        return array


def on_device(
    noisy_embed, self_cond, cond_flag, timestep, in_weight, qkv_weight, out_weight,
    up_weight, up_bias, down_weight, ada_weight, norm_gain, norm_bias, out_grad,
):
    links = Links()
    n_t = links.n_t
    rows, features = out_grad.shape
    embed_cols = noisy_embed.shape[1]
    seq_len = rows * n_t // cond_flag.shape[0]
    assert seq_len == 2 * rows
    head_cols = qkv_weight.shape[2]
    hidden_cols = up_weight.shape[1]

    sequence = (links.tensor * rows) // seq_len
    flag = pick(cond_flag, sequence).astype(f32)
    embed_low = time_embed(lax.dynamic_slice_in_dim(timestep, sequence, 1, 0), ada_weight.shape[0]).astype(bf16)
    ada = jnp.dot(embed_low, ada_weight, preferred_element_type=f32)
    shift, scale, gate = ada[:, :features], 1.0 + ada[:, features : 2 * features], ada[:, 2 * features :]

    joined = jnp.concatenate([noisy_embed, (self_cond.astype(f32) * flag).astype(bf16)], axis=1)
    attn_quarter = jnp.concatenate([qkv_weight[0].T, qkv_weight[1].T, qkv_weight[2].T, out_weight])
    joined_far, bias_all, attn_all, ups, downs = gather(
        joined, up_bias.astype(f32)[None], (attn_quarter, up_weight, down_weight)
    )
    attn_all = attn_all.reshape(n_t, 4, head_cols, features)
    attn_weights = [attn_all[:, m].reshape(n_t * head_cols, features) for m in range(4)]
    joined = jnp.concatenate([joined, joined_far])
    cosine, sine = rope_tables(seq_len, (links.tensor * rows) % seq_len)
    hidden = jnp.dot(joined, in_weight, preferred_element_type=f32)
    normed_one, inverse_one = norm_stats(hidden)
    attn_in = (normed_one * norm_gain + norm_bias).astype(bf16)
    q, k, v, mixed, mixed_full, log_total = attend(attn_in, attn_all, cosine, sine, rows)
    resid = hidden[:rows] + nn(mixed, attn_weights[3])
    normed_two, inverse_two = norm_stats(resid)
    modulated = (scale * normed_two + shift).astype(bf16)
    pre = jnp.einsum("td,kdh->kth", modulated, ups, preferred_element_type=f32) + bias_all
    act, slope = gelu_both(pre)
    act = act.astype(bf16)
    branch = jnp.einsum("kth,khd->td", act, downs, preferred_element_type=f32)
    result = resid + gate * branch

    grad_branch = (gate * out_grad).astype(bf16)
    grad_down = jnp.einsum("kth,td->khd", act, grad_branch, preferred_element_type=f32).astype(bf16)
    grad_act = jnp.einsum("td,khd->kth", grad_branch, downs, preferred_element_type=f32)
    grad_pre = (slope * grad_act).astype(bf16)
    grad_bias = jnp.sum(grad_pre.astype(f32), axis=1)
    grad_up = jnp.einsum("td,kth->kdh", modulated, grad_pre, preferred_element_type=f32).astype(bf16)
    grad_mod = jnp.einsum("kth,kdh->td", grad_pre, ups, preferred_element_type=f32)

    grad_resid = out_grad + norm_back(normed_two, inverse_two, scale * grad_mod)
    grad_ada_row = jnp.concatenate(
        [
            jnp.sum(grad_mod, axis=0),
            jnp.sum(grad_mod * normed_two, axis=0),
            jnp.sum(out_grad * branch, axis=0),
            embed_low[0].astype(f32),
        ]
    )[None]
    ada_rows = links.gather_all(grad_ada_row)
    grad_ada = lax.dot_general(
        ada_rows[:, 3 * features :], ada_rows[:, : 3 * features],
        (((0,), (0,)), ((), ())), precision=precise, preferred_element_type=f32,
    )

    grad_attn = grad_resid.astype(bf16)
    grad_out_w = tn(mixed, grad_attn).astype(bf16)
    grad_mixed = nt(grad_attn, attn_weights[3]).astype(bf16)
    grad_q, grad_k, grad_v = attend_back(q, k, v, grad_mixed, mixed_full, log_total, cosine, sine)
    grad_q_w = tn(grad_q, attn_in[:rows]).astype(bf16)
    grad_k_w = tn(grad_k, attn_in).astype(bf16)
    grad_v_w = tn(grad_v, attn_in).astype(bf16)
    grad_down, grad_up, grad_attn_w = reduce_all(grad_down, grad_up, (grad_q_w, grad_k_w, grad_v_w, grad_out_w))
    grad_down = grad_down.reshape(hidden_cols, features).astype(f32)
    grad_up = grad_up.reshape(features, hidden_cols).astype(f32)
    grad_attn_w = grad_attn_w.reshape(4, head_cols, features).astype(f32)
    grad_qkv, grad_out = jnp.swapaxes(grad_attn_w[:3], 1, 2), grad_attn_w[3]

    grad_norm = nn(grad_k, attn_weights[1]) + nn(grad_v, attn_weights[2])
    grad_norm = jnp.concatenate([grad_norm[:rows] + nn(grad_q, attn_weights[0]), grad_norm[rows:]])
    grad_gain = jnp.sum(grad_norm * normed_one, axis=0)
    grad_offset = jnp.sum(grad_norm, axis=0)
    grad_hidden = norm_back(normed_one, inverse_one, grad_norm * norm_gain)
    grad_hidden = jnp.concatenate([grad_hidden[:rows] + grad_resid, grad_hidden[rows:]]).astype(bf16)
    grad_in = tn(joined, grad_hidden)
    grad_joined = nt(grad_hidden, in_weight)
    grad_joined = grad_joined[:rows] + links.swap(grad_joined[rows:], 0, 1)
    grad_noisy = grad_joined[:, :embed_cols]
    grad_self = grad_joined[:, embed_cols:] * flag

    bias_rows = jnp.stack([pick(grad_bias, links.tensor ^ t) for t in range(n_t)]).reshape(-1, features)
    small = links.add_all(jnp.concatenate([grad_in, grad_gain[None], grad_offset[None], bias_rows]))
    n_in = grad_in.shape[0]
    grad_in, grad_gain, grad_offset = small[:n_in], small[n_in], small[n_in + 1]
    grad_bias = pick(small[n_in + 2 :].reshape(n_t, hidden_cols), links.tensor)
    return (
        result, grad_noisy, grad_self, grad_in, grad_qkv, grad_out, grad_up,
        grad_bias, grad_down, grad_ada, grad_gain, grad_offset,
    )


def solution(mesh):
    tokens = P(("dp", "tensor"), None)
    return jax.shard_map(
        on_device,
        mesh=mesh,
        in_specs=(
            tokens, tokens, P("dp"), P("dp"), P(), P(None, None, "tensor"), P("tensor", None),
            P(None, "tensor"), P("tensor"), P("tensor", None), P(), P(), P(), tokens,
        ),
        out_specs=(
            tokens, tokens, tokens, P(), P(None, None, "tensor"), P("tensor", None), P(None, "tensor"),
            P("tensor"), P("tensor", None), P(), P(), P(),
        ),
        check_vma=False,
    )
```

```python
import functools
import math

import jax
import jax.numpy as jnp
import numpy as np
from jax import lax
from jax.experimental import pallas as pl
from jax.experimental.pallas import tpu as pltpu
from jax.sharding import PartitionSpec as P

HD = 64
SPLIT = 8
norm_epsilon = 1e-05
precise = lax.Precision.HIGHEST
f32, bf16 = jnp.float32, jnp.bfloat16
MESH = pl.DeviceIdType.MESH


def nt(left, right):
    return lax.dot_general(left, right, (((1,), (1,)), ((), ())), preferred_element_type=f32)


def nn(left, right):
    return lax.dot_general(left, right, (((1,), (0,)), ((), ())), preferred_element_type=f32)


def tn(left, right):
    return lax.dot_general(left, right, (((0,), (0,)), ((), ())), preferred_element_type=f32)


def swap_halves(values):
    width = values.shape[1]
    lane = lax.broadcasted_iota(jnp.int32, values.shape, 1)
    return jnp.where(
        lane % HD < HD // 2,
        pltpu.roll(values, width - HD // 2, 1),
        pltpu.roll(values, HD // 2, 1),
    )


def norm_stats(values):
    center = jnp.mean(values, axis=-1, keepdims=True)
    spread = values - center
    second = jnp.mean(spread * spread, axis=-1, keepdims=True)
    inverse = lax.rsqrt(second + norm_epsilon)
    return spread * inverse, inverse


def norm_back(normed, inverse, upstream):
    first = jnp.mean(upstream, axis=-1, keepdims=True)
    cross = jnp.mean(upstream * normed, axis=-1, keepdims=True)
    return (upstream - first - normed * cross) * inverse


def rope_tables(length, first):
    halfway = HD // 2
    freqs = np.exp(-np.float32(math.log(10000.0)) * np.arange(halfway, dtype=np.float32) * np.float32(2.0 / HD))
    angle = np.arange(length, dtype=np.float32)[:, None] * freqs[None, :].astype(np.float32)
    cosine, sine = np.cos(angle), np.sin(angle)
    both = np.concatenate([np.tile(cosine, (1, 4)), np.tile(np.concatenate([-sine, sine], 1), (1, 2))], 1)
    both = jnp.asarray(np.concatenate([both, both], 0).astype(np.float32))
    both = lax.dynamic_slice_in_dim(both, first, length, 0)
    return both[:, :128], both[:, 128:]


def time_embed(steps, channels):
    halfway = channels // 2
    freqs = jnp.exp(-math.log(10000.0) * jnp.arange(halfway, dtype=f32) * (1.0 / halfway))
    angle = steps.astype(f32)[:, None] * freqs[None, :]
    return jnp.concatenate([jnp.cos(angle), jnp.sin(angle)], axis=1)


def gelu_both(values):
    phi = 0.5 * (1.0 + lax.erf(values * math.sqrt(0.5)))
    bell = jnp.exp(-0.5 * values * values) * (1.0 / math.sqrt(2.0 * math.pi))
    return values * phi, phi + values * bell


def pick(array, index, axis=0):
    return lax.dynamic_index_in_dim(array, index, axis, keepdims=False)


def flip(index, bits):
    bit = 1
    while bit <= bits:
        if bits & bit:
            index = index + bit - 2 * bit * ((index // bit) % 2)
        bit *= 2
    return index


class Net:
    def __init__(self, n_dp, n_t, send_sems, recv_sems):
        self.dp, self.tensor = lax.axis_index("dp"), lax.axis_index("tensor")
        self.low = self.dp % SPLIT
        self.core, self.x, self.y = self.low % 2, (self.low // 2) % 2, self.low // 4
        self.n_t, self.high_bits = n_t, []
        while SPLIT << len(self.high_bits) < n_dp:
            self.high_bits.append(SPLIT << len(self.high_bits))
        self.sems, self.used = (send_sems, recv_sems), 0

    def peers(self):
        return [(b, 0) for b in [1, 2, 4] + self.high_bits] + [(0, k) for k in range(1, self.n_t)]

    def peer(self, bits):
        return {"dp": flip(self.dp, bits[0]), "tensor": flip(self.tensor, bits[1])}

    def barrier(self):
        ready = pltpu.get_barrier_semaphore()
        for bits in self.peers():
            pl.semaphore_signal(ready, inc=1, device_id=self.peer(bits), device_id_type=MESH)
        pl.semaphore_wait(ready, len(self.peers()))

    def send(self, source, target, bits):
        copy = pltpu.make_async_remote_copy(
            src_ref=source, dst_ref=target,
            send_sem=self.sems[0].at[self.used], recv_sem=self.sems[1].at[self.used],
            device_id=self.peer(bits), device_id_type=MESH,
        )
        self.used += 1
        return copy

    def local(self, source, target):
        copy = pltpu.make_async_copy(source, target, self.sems[0].at[self.used])
        self.used += 1
        return copy


def rows_of(piece, rows):
    return pl.ds(pl.multiple_of(piece * rows, rows), rows)


def start_all(*copies):
    for copy in copies:
        copy.start()


def arrived(*copies):
    for copy in copies:
        copy.wait_recv()


def sent(*copies):
    for copy in copies:
        copy.wait_send()


def gather_steps(net, quarter, full, kept):
    rows, half, low = quarter.shape[0] // SPLIT, quarter.shape[1] // 2, net.low
    far, cols = pl.ds(1, net.n_t - 1), (pl.ds(0, half), pl.ds(half, half))
    mine, from_x, from_y, from_xy = (rows_of(flip(low, bits), rows) for bits in (0, 2, 4, 6))
    by_z = [net.send(quarter.at[mine], full.at[k, mine], (0, k)) for k in range(1, net.n_t)]
    block = full.at[far, mine]
    to_x, to_y = net.send(block, block, (2, 0)), net.send(block, block, (4, 0))
    part = full.at[far, from_x, cols[0]]
    x_to_y = net.send(part, part, (4, 0))
    part = full.at[far, from_y, cols[1]]
    y_to_x = net.send(part, part, (2, 0))
    to_core = []
    for where in (mine, from_x, from_y, from_xy):
        block = full.at[far, where]
        to_core.append(net.send(block, block, (1, 0)))
    own = net.local(quarter, full.at[0])
    keep = net.local(full, kept)

    def start():
        start_all(*by_z, own)

    def plane():
        arrived(*by_z)
        start_all(to_x, to_y, to_core[0])

    def relay():
        arrived(to_x)
        start_all(x_to_y, to_core[1])
        arrived(to_y)
        start_all(y_to_x, to_core[2])

    def across():
        arrived(x_to_y, y_to_x)
        start_all(to_core[3])

    def finish():
        arrived(*to_core)
        own.wait()
        keep.start()
        sent(*by_z, to_x, to_y, x_to_y, y_to_x, *to_core)

    return [start, plane, relay, across, finish], keep


def collect_steps(net, out):
    half, low = out.shape[2] // 2, net.low
    mine, from_x, from_y, from_xy = (flip(low, bits) for bits in (0, 2, 4, 6))
    to_x, to_y = net.send(out.at[mine], out.at[mine], (2, 0)), net.send(out.at[mine], out.at[mine], (4, 0))
    part = out.at[from_x, :, pl.ds(0, half)]
    x_to_y = net.send(part, part, (4, 0))
    part = out.at[from_y, :, pl.ds(half, half)]
    y_to_x = net.send(part, part, (2, 0))
    to_core = [net.send(out.at[where], out.at[where], (1, 0)) for where in (mine, from_x, from_y, from_xy)]

    def start():
        start_all(to_x, to_y, to_core[0])

    def relay():
        arrived(to_x)
        start_all(x_to_y, to_core[1])
        arrived(to_y)
        start_all(y_to_x, to_core[2])

    def across():
        arrived(x_to_y, y_to_x)
        start_all(to_core[3])

    def finish():
        arrived(*to_core)
        sent(to_x, to_y, x_to_y, y_to_x, *to_core)

    return [start, relay, across, finish]


ANY = pl.BlockSpec(memory_space=pl.ANY)
VMEM = pl.BlockSpec(memory_space=pltpu.VMEM)


def loop(count, body):
    def step(i, carry):
        body(i)
        return carry

    lax.fori_loop(0, count, step, 0)


def loop_with(count, body, steps):
    def step(i):
        body(i)
        for turn, act in steps:
            pl.when(i == turn)(act)

    loop(count, step)


def forward_kernel(
    n_dp, n_t,
    joined_ref, bias_ref, a_ref, u_ref, d_ref, in_ref, gain_ref, offset_ref, cos_ref, sin_ref, embed_ref, ada_ref, og_ref,
    result_ref, joined_all_ref, gate_row_ref, ada_row_ref,
    a_out, u_out, d_out, attn_out, q_out, k_out, v_out, m_out, mf_out, l_out,
    resid_out, mod_out, act_out, slope_out, gb_out,
    a_s, u_s, d_s, joined_s, bias_s, attn_in, q_s, k_s, v_s, m_s, mf_s, l_s, resid, mod_s, act_s, slope_s, gb_s, branch, hidden,
    send_sems, recv_sems,
):
    net = Net(n_dp, n_t, send_sems, recv_sems)
    rows, features = og_ref.shape
    head_cols = features // n_t
    a, a_keep = gather_steps(net, a_ref, a_s, a_out)
    u, u_keep = gather_steps(net, u_ref, u_s, u_out)
    d, d_keep = gather_steps(net, d_ref, d_s, d_out)
    far_rows = joined_s.at[pl.ds(rows, rows)]
    joined_copy = net.send(joined_ref, far_rows, (0, 1))
    bias_copies = [net.send(bias_ref, bias_s.at[k], (0, k)) for k in range(1, n_t)]
    kept = [
        net.local(source, target)
        for source, target in (
            (attn_in, attn_out), (q_s, q_out), (k_s, k_out), (v_s, v_out), (m_s, m_out),
            (mf_s, mf_out), (l_s, l_out), (resid, resid_out), (mod_s, mod_out), (act_s, act_out),
            (slope_s, slope_out), (gb_s, gb_out),
        )
    ]
    net.barrier()
    start_all(joined_copy, *bias_copies)
    a[0]()
    bias_s[0] = bias_ref[...]
    joined_s[pl.ds(0, rows), :] = joined_ref[...]
    chunk = 256

    def norm_rows(i, own):
        where = pl.ds(pl.multiple_of(i * chunk, chunk), chunk)
        values = nn(joined_s[where, :], in_ref[...])
        if own:
            hidden[where, :] = values
        attn_in[where, :] = (norm_stats(values)[0] * gain_ref[...] + offset_ref[...]).astype(bf16)

    loop(rows // chunk, lambda i: norm_rows(i, True))
    ada = nn(embed_ref[...], ada_ref[...])[0:1]
    ada_row_ref[...] = ada
    shift, scale, gate = ada[:, :features], 1.0 + ada[:, features : 2 * features], ada[:, 2 * features :]
    gb_s[...] = (gate * og_ref[...]).astype(bf16)
    a[1]()
    u[0]()
    arrived(joined_copy)
    joined_all_ref[...] = joined_s[...]
    loop(rows // chunk, lambda i: norm_rows(i + rows // chunk, False))
    a[2]()
    u[1]()
    d[0]()
    a[3]()
    a[4]()

    def project(i):
        wide = 2 * head_cols
        weight = lambda m: a_s[pl.ds(2 * i, 2), pl.ds(m * head_cols, head_cols), :].reshape(wide, features)
        cosine = jnp.concatenate([cos_ref[...]] * (wide // 128), axis=1)
        sine = jnp.concatenate([sin_ref[...]] * (wide // 128), axis=1)
        proj = nt(attn_in[pl.ds(0, rows), :], weight(0))
        query = ((proj * cosine[:rows] + swap_halves(proj) * sine[:rows]) * HD**-0.5).astype(bf16)
        proj = nt(attn_in[...], weight(1))
        key = (proj * cosine + swap_halves(proj) * sine).astype(bf16)
        value = nt(attn_in[...], weight(2)).astype(bf16)
        for pair in range(wide // 128):
            where = i * (wide // 128) + pair
            cols = slice(pair * 128, (pair + 1) * 128)
            q_s[where], k_s[where], v_s[where] = query[:, cols], key[:, cols], value[:, cols]

    loop_with(n_t // 2, project, [(0, u[2]), (1, d[1])])
    lane = lax.broadcasted_iota(jnp.int32, (rows, 128), 1)

    def attend(pair):
        keys, values, queries = k_s[pair], v_s[pair], q_s[pair]
        out = stat = None
        for head in range(2):
            scores = nt(jnp.where(lane // HD == head, queries, jnp.zeros_like(queries)), keys)
            top = jnp.max(scores, axis=1, keepdims=True)
            probs = jnp.exp(scores - top)
            total = jnp.sum(probs, axis=1, keepdims=True)
            mixed = nn(probs.astype(bf16), values) * (1.0 / total)
            log_total = jnp.broadcast_to(top + jnp.log(total), (rows, 128))
            out = mixed if head == 0 else jnp.where(lane < HD, out, mixed)
            stat = log_total if head == 0 else jnp.where(lane < HD, stat, log_total)
        m_s[pair] = out.astype(bf16)
        mf_s[pair] = out
        l_s[pair] = stat

    n_pairs = features // 128
    loop_with(n_pairs, attend, [(0, u[3]), (1, u[4]), (3, d[2]), (5, d[3])])
    start_all(*kept[:7])
    out_weight = a_s[:, pl.ds(3 * head_cols, head_cols), :].reshape(features, features)
    mixed = jnp.concatenate([m_s[pair] for pair in range(n_pairs)], axis=1)
    resid[...] = hidden[...] + nn(mixed, out_weight)

    def norm_again(i):
        where = pl.ds(pl.multiple_of(i * chunk, chunk), chunk)
        mod_s[where, :] = (scale * norm_stats(resid[where, :])[0] + shift).astype(bf16)

    loop(rows // chunk, norm_again)
    start_all(*kept[7:9])
    arrived(*bias_copies)

    def up(i):
        k, where = i // 2, pl.ds(pl.multiple_of((i % 2) * (rows // 2), rows // 2), rows // 2)
        pre = nn(mod_s[where, :], u_s[k]) + bias_s[k]
        act, slope = gelu_both(pre)
        act_s[k, where, :] = act.astype(bf16)
        slope_s[k, where, :] = slope.astype(bf16)

    loop(2 * n_t, up)
    start_all(*kept[9:])
    d[4]()
    branch[...] = jnp.zeros_like(branch)

    def down(k):
        branch[...] += nn(act_s[k], d_s[k])

    loop(n_t, down)
    result_ref[...] = resid[...] + gate * branch[...]
    gate_row_ref[...] = jnp.sum(og_ref[...] * branch[...], axis=0, keepdims=True)
    for copy in kept + [a_keep, u_keep, d_keep]:
        copy.wait()
    sent(joined_copy, *bias_copies)


def forward(joined, bias, quarters, in_weight, gain, offset, cosine, sine, embed, ada_weight, out_grad):
    n_dp, n_t = lax.axis_size("dp"), lax.axis_size("tensor")
    (rows, features), length = out_grad.shape, cosine.shape[0]
    pairs, hidden_cols = features // 128, quarters[1].shape[1]
    shape = jax.ShapeDtypeStruct
    kept = [((n_t,) + w.shape, bf16) for w in quarters] + [
        ((length, features), bf16),
        ((pairs, rows, 128), bf16), ((pairs, length, 128), bf16), ((pairs, length, 128), bf16),
        ((pairs, rows, 128), bf16), ((pairs, rows, 128), f32), ((pairs, rows, 128), f32),
        ((rows, features), f32), ((rows, features), bf16),
        ((n_t, rows, hidden_cols), bf16), ((n_t, rows, hidden_cols), bf16), ((rows, features), bf16),
    ]
    scratch = kept[:3] + [((length, joined.shape[1]), bf16), ((n_t,) + bias.shape, f32)] + kept[3:]
    return pl.pallas_call(
        functools.partial(forward_kernel, n_dp, n_t),
        in_specs=[VMEM] * 13,
        out_specs=[VMEM] * 4 + [ANY] * len(kept),
        out_shape=[
            shape((rows, features), f32), shape((length, joined.shape[1]), bf16), shape((1, features), f32),
            shape((1, ada_weight.shape[1]), f32),
        ] + [shape(*item) for item in kept],
        scratch_shapes=[pltpu.VMEM(*item) for item in scratch]
        + [pltpu.VMEM((rows, features), f32)] * 2
        + [pltpu.SemaphoreType.DMA((64,))] * 2,
        compiler_params=pltpu.CompilerParams(collective_id=0, has_side_effects=True, vmem_limit_bytes=63 << 20),
        name="forward",
    )(joined, bias, *quarters, in_weight, gain, offset, cosine, sine, embed, ada_weight, out_grad)


def reduce_buffers(n_t, rows, cols, n_high):
    half = cols // 2
    kinds = [
        (n_t, 2, 2, rows, cols), (n_t, 2, rows, half), (n_t, 2, rows, half), (n_t, rows, half), (n_t, rows, half),
        (n_t, rows, cols), (n_t, rows, cols), (n_high + 1, rows, cols),
    ]
    return [pltpu.VMEM(shape, bf16) for shape in kinds]


def reduce_steps(net, terms, buffers, out):
    came, by_x, by_y, then_y, then_x, summed, away, more = buffers
    half = terms.shape[5] // 2
    first, second = pl.ds(0, half), pl.ds(half, half)
    n_t, x, y, core = net.n_t, net.x, net.y, net.core
    there = net.send(terms.at[:, :, :, 1 - core], came, (1, 0))
    to_x = net.send(terms.at[:, :, 1 - x, core, :, first], by_x, (2, 0))
    to_y = net.send(terms.at[:, 1 - y, :, core, :, second], by_y, (4, 0))
    x_then_y = net.send(by_x.at[:, 1 - y], then_y, (4, 0))
    y_then_x = net.send(by_y.at[:, 1 - x], then_x, (2, 0))
    by_z = [net.send(summed.at[k], away.at[k], (0, k)) for k in range(1, n_t)]
    by_high = [net.send(more.at[0], more.at[n + 1], (bit, 0)) for n, bit in enumerate(net.high_bits)]
    collect = collect_steps(net, out)

    def start():
        there.start()

    def add_core():
        arrived(there)

        def add(i):
            k, j = i // 4, i % 4
            total = terms[k, j // 2, j % 2, core].astype(f32) + came[k, j // 2, j % 2].astype(f32)
            terms[k, j // 2, j % 2, core] = total.astype(bf16)

        loop(4 * n_t, add)
        start_all(to_x, to_y)

    def add_first():
        arrived(to_x, to_y)

        def add(i):
            k, j = i // 2, i % 2
            by_x[k, j] = (terms[k, j, x, core, :, first].astype(f32) + by_x[k, j].astype(f32)).astype(bf16)
            by_y[k, j] = (terms[k, y, j, core, :, second].astype(f32) + by_y[k, j].astype(f32)).astype(bf16)

        loop(2 * n_t, add)
        start_all(x_then_y, y_then_x)
        sent(there, to_x, to_y)

    def add_second():
        arrived(x_then_y, y_then_x)

        def add(k):
            summed[k, :, first] = (by_x[k, y].astype(f32) + then_y[k].astype(f32)).astype(bf16)
            summed[k, :, second] = (by_y[k, x].astype(f32) + then_x[k].astype(f32)).astype(bf16)

        loop(n_t, add)
        start_all(*by_z)
        sent(x_then_y, y_then_x)

    def add_tensor():
        arrived(*by_z)
        total = summed[0].astype(f32)
        for k in range(1, n_t):
            total = total + away[k].astype(f32)
        for n, copy in enumerate(by_high):
            more[0] = total.astype(bf16)
            copy.start()
            arrived(copy)
            sent(copy)
            total = total + more[n + 1].astype(f32)
        out[net.low] = total.astype(bf16)
        sent(*by_z)
        collect[0]()

    return [start, add_core, add_first, add_second, add_tensor] + collect[1:]


def backward_kernel(
    n_dp, n_t,
    joined_ref, in_ref, gain_ref, cos_ref, sin_ref, ada_ref, gate_row_ref, embed_ref, og_ref, gb_ref, mod_ref, resid_ref,
    act_ref, slope_ref, u_ref, d_ref, a_ref, q_ref, k_ref, v_ref, m_ref, mf_ref, l_ref, attn_ref,
    d_out, u_out, a_out, small_out, rows_out, gj_out,
    terms_da, terms_u, act_b, slope_b, d_b, u_b, grad, grad_low, out_terms, g_s, q_b, k_b, v_b, mf_b, l_b, m_s, attn_s,
    dq_s, dk_s, dv_s, acc_k, acc_v, small_b, gj_s, gj_far, *scratch,
):
    send_sems, recv_sems, load_sems = scratch[-3:]
    net = Net(n_dp, n_t, send_sems, recv_sems)
    rows, features = og_ref.shape
    length, head_cols = joined_ref.shape[0], features // n_t
    n_pairs, chunk, n_in = features // 128, 256, joined_ref.shape[1]
    n_buf = (len(scratch) - 3) // 2
    d = reduce_steps(net, terms_da, scratch[:n_buf], d_out)
    u = reduce_steps(net, terms_u, scratch[n_buf : 2 * n_buf], u_out)
    a = reduce_steps(net, terms_da, scratch[:n_buf], a_out)

    def stream(first_sem, *pairs):
        copies = lambda i: [
            pltpu.make_async_copy(source.at[i], target.at[i % 2], load_sems.at[first_sem + 2 * n + i % 2])
            for n, (source, target) in enumerate(pairs)
        ]
        return (lambda i: start_all(*copies(i))), (lambda i: [copy.wait() for copy in copies(i)])

    def streamed(count, start, wait, body, steps):
        def turn(i):
            pl.when(i + 1 < count)(lambda: start(i + 1))
            wait(i)
            body(i)

        loop_with(count, turn, steps)

    act_start, act_wait = stream(0, (act_ref, act_b))
    ff_start, ff_wait = stream(2, (slope_ref, slope_b), (d_ref, d_b), (u_ref, u_b))
    at_start, at_wait = stream(8, (q_ref, q_b), (k_ref, k_b), (v_ref, v_b), (mf_ref, mf_b), (l_ref, l_b))
    load_m = pltpu.make_async_copy(m_ref, m_s, load_sems.at[18])
    load_attn = pltpu.make_async_copy(attn_ref, attn_s, load_sems.at[19])
    weights = [(d_b, 0), (d_b, 1), (u_b, 0), (u_b, 1)]
    load_w = [
        [
            pltpu.make_async_copy(
                a_ref.at[k, pl.ds(m * head_cols, head_cols)], ref.at[slot, pl.ds(k * head_cols, head_cols)],
                load_sems.at[20 + m * n_t + k],
            )
            for k in range(n_t)
        ]
        for m, (ref, slot) in enumerate(weights)
    ]
    bits = [(0, 1 << b) for b in range((n_t - 1).bit_length())] + [(b, 0) for b in [1, 2, 4] + net.high_bits]
    row_copies = [
        net.send(rows_out.at[pl.ds(0, 1 << n)], rows_out.at[pl.ds(1 << n, 1 << n)], bit) for n, bit in enumerate(bits)
    ]
    sum_copies = [net.send(small_b.at[2 * n], small_b.at[2 * n + 1], bit) for n, bit in enumerate(bits)]
    gj_copy = net.send(gj_s.at[pl.ds(rows, rows)], gj_far, (0, 1))

    def row_step(n):
        def step():
            if n:
                arrived(row_copies[n - 1])
            if n < len(bits):
                row_copies[n].start()

        return step

    def sum_step(n):
        def step():
            arrived(sum_copies[n - 1])
            total = small_b[2 * n - 2] + small_b[2 * n - 1]
            if n < len(bits):
                small_b[2 * n] = total
                sum_copies[n].start()
            else:
                small_out[...] = total

        return step

    act_start(0)
    ff_start(0)
    load_m.start()
    load_attn.start()
    net.barrier()
    scale = 1.0 + ada_ref[:, features : 2 * features]
    gb = gb_ref[...]

    def down_terms(k):
        terms = tn(act_b[k % 2], gb).astype(bf16)
        terms_da[k] = terms.reshape(terms_da.shape[1:])

    streamed(n_t, act_start, act_wait, down_terms, [])
    d[0]()
    grad[...] = jnp.zeros_like(grad)
    small_b[0] = jnp.zeros(small_b.shape[1:], f32)

    def ff_back(k):
        slot = k % 2
        grad_pre = (slope_b[slot].astype(f32) * nt(gb, d_b[slot])).astype(bf16)
        place = n_in + 2 + net.tensor
        bit = 1
        while bit < n_t:
            place = place + jnp.where((k // bit) % 2 == 1, flip(net.tensor, bit) - net.tensor, 0)
            bit *= 2
        small_b[0, pl.ds(place, 1), :] = jnp.sum(grad_pre.astype(f32), axis=0, keepdims=True)
        terms_u[k] = tn(mod_ref[...], grad_pre).astype(bf16).reshape(terms_u.shape[1:])
        grad[...] += nt(grad_pre, u_b[slot])

    streamed(n_t, ff_start, ff_wait, ff_back, [(1, d[1])])
    u[0]()
    for copies in load_w[::-1]:
        start_all(*copies)
    at_start(0)
    shift_row = scale_row = 0.0
    for i in range(rows // chunk):
        where = pl.ds(i * chunk, chunk)
        upstream = grad[where, :]
        normed, inverse = norm_stats(resid_ref[where, :])
        shift_row += jnp.sum(upstream, axis=0, keepdims=True)
        scale_row += jnp.sum(upstream * normed, axis=0, keepdims=True)
        total = og_ref[where, :] + norm_back(normed, inverse, scale * upstream)
        grad[where, :] = total
        grad_low[where, :] = total.astype(bf16)
    row = jnp.concatenate([shift_row, scale_row, gate_row_ref[...], embed_ref[0:1, :].astype(f32)], axis=1)
    for i in range(row.shape[1] // 128):
        rows_out[0, i : i + 1, :] = row[:, i * 128 : (i + 1) * 128]
    row_step(0)()
    load_m.wait()
    for copy in load_w[3]:
        copy.wait()
    join = lambda ref, where: jnp.concatenate([ref[pair, where, :] for pair in range(n_pairs)], axis=1)
    own = pl.ds(0, rows)
    out_terms[...] = tn(join(m_s, own), grad_low[...]).astype(bf16)
    grad_mixed = nt(grad_low[...], u_b[1]).astype(bf16)
    for pair in range(n_pairs):
        g_s[pair] = grad_mixed[:, pair * 128 : (pair + 1) * 128]
    d[2]()

    def attend_back(pair):
        slot = pair % 2
        keys, values, queries, grads = k_b[slot], v_b[slot], q_b[slot], g_s[pair]
        lane = lax.broadcasted_iota(jnp.int32, queries.shape, 1)
        product = grads.astype(f32) * mf_b[slot]
        grad_q = None
        for head in range(2):
            mine = lane // HD == head
            q_head = jnp.where(mine, queries, jnp.zeros_like(queries))
            g_head = jnp.where(mine, grads, jnp.zeros_like(grads))
            center = jnp.sum(jnp.where(mine, product, 0.0), axis=1, keepdims=True)
            probs = jnp.exp(nt(q_head, keys) - l_b[slot, :, pl.ds(head * HD, 1)])
            grad_prob = nt(g_head, values)
            grad_score = (probs * (grad_prob - center)).astype(bf16)
            part = nn(grad_score, keys) * HD**-0.5
            grad_q = part if head == 0 else jnp.where(lane < HD, grad_q, part)
            part_v = tn(probs.astype(bf16), g_head)
            part_k = tn(grad_score, q_head)
            if head == 0:
                acc_k[...] = part_k
                acc_v[...] = part_v
            else:
                dk = acc_k[...] + part_k
                dv = acc_v[...] + part_v
        cosine, sine = cos_ref[own, :], sin_ref[own, :]
        dq_s[pair] = (grad_q * cosine + swap_halves(grad_q * sine)).astype(bf16)
        dk_s[pair] = (dk * cos_ref[...] + swap_halves(dk * sin_ref[...])).astype(bf16)
        dv_s[pair] = dv.astype(bf16)

    steps = [(0, u[1]), (1, d[3]), (4, u[2]), (5, d[4])]
    steps += [(min(n, n_pairs - 1), row_step(n + 1)) for n in range(len(bits))]
    streamed(n_pairs, at_start, at_wait, attend_back, steps)
    load_attn.wait()
    every = pl.ds(0, length)
    d[5]()
    q_terms = tn(join(dq_s, own), attn_s[own, :]).astype(bf16)
    u[3]()
    d[6]()
    k_terms = tn(join(dk_s, every), attn_s[...]).astype(bf16)
    d[7]()
    v_terms = tn(join(dv_s, every), attn_s[...]).astype(bf16)
    for m, terms in enumerate((q_terms, k_terms, v_terms, out_terms[...])):
        for k in range(n_t):
            block = terms[k * head_cols : (k + 1) * head_cols]
            terms_da[k, m // 2, m % 2] = block.reshape(terms_da.shape[3:])
    a[0]()
    u[4]()
    for copies in load_w[:3]:
        for copy in copies:
            copy.wait()

    def norm_grads(i, mine):
        where = pl.ds(pl.multiple_of(i * chunk, chunk), chunk)
        tokens = joined_ref[where, :]
        normed, inverse = norm_stats(nn(tokens, in_ref[...]))
        total = nn(join(dk_s, where), d_b[1]) + nn(join(dv_s, where), u_b[0])
        if mine:
            total = total + nn(join(dq_s, where), d_b[0])
        small_b[0, n_in : n_in + 1, :] += jnp.sum(total * normed, axis=0, keepdims=True)
        small_b[0, n_in + 1 : n_in + 2, :] += jnp.sum(total, axis=0, keepdims=True)
        upstream = norm_back(normed, inverse, total * gain_ref[...])
        if mine:
            upstream = upstream + grad[where, :]
        upstream = upstream.astype(bf16)
        small_b[0, 0:n_in, :] += tn(tokens, upstream)
        gj_s[where, :] = nt(upstream, in_ref[...])

    per = rows // chunk
    loop(per, lambda i: norm_grads(i + per, False))
    gj_copy.start()
    a[1]()
    u[5]()
    loop(per, lambda i: norm_grads(i, True))
    sum_copies[0].start()
    u[6]()
    u[7]()
    tail = [a[2], a[3], a[4], a[5], a[6], a[7]]
    for n in range(max(len(tail), len(bits))):
        if n < len(bits):
            sum_step(n + 1)()
        if n < len(tail):
            tail[n]()
    arrived(gj_copy)
    gj_out[...] = gj_s[own, :] + gj_far[...]
    sent(gj_copy, *row_copies, *sum_copies)


def backward(small_inputs, large_inputs, n_joined):
    n_dp, n_t = lax.axis_size("dp"), lax.axis_size("tensor")
    og, resid = small_inputs[8], small_inputs[11]
    (rows, features), length = og.shape, small_inputs[3].shape[0]
    hidden_cols = large_inputs[2].shape[2]
    pairs, part, n_high = features // 128, features // SPLIT, (n_dp // SPLIT).bit_length() - 1
    n_bits = (n_dp * n_t).bit_length() - 1
    n_small = -(-(n_joined + 2 + n_t) // 8) * 8
    row_tiles = (small_inputs[5].shape[1] + small_inputs[7].shape[1]) // 128
    shape = jax.ShapeDtypeStruct
    terms = (n_t, 2, 2, 2, part, features)
    scratch = [
        (terms, bf16), (terms, bf16), ((2, rows, hidden_cols), bf16), ((2, rows, hidden_cols), bf16),
        ((2, hidden_cols, features), bf16), ((2, features, hidden_cols), bf16), ((rows, features), f32),
        ((rows, features), bf16), ((features, features), bf16), ((pairs, rows, 128), bf16),
        ((2, rows, 128), bf16), ((2, length, 128), bf16), ((2, length, 128), bf16), ((2, rows, 128), f32),
        ((2, rows, 128), f32), ((pairs, rows, 128), bf16), ((length, features), bf16),
        ((pairs, rows, 128), bf16), ((pairs, length, 128), bf16), ((pairs, length, 128), bf16),
        ((length, 128), f32), ((length, 128), f32), ((2 * n_bits, n_small, features), f32),
        ((length, n_joined), f32), ((rows, n_joined), f32),
    ]
    return pl.pallas_call(
        functools.partial(backward_kernel, n_dp, n_t),
        in_specs=[VMEM] * len(small_inputs) + [ANY] * len(large_inputs),
        out_specs=[VMEM] * 6,
        out_shape=[shape((SPLIT, part, features), bf16)] * 3
        + [
            shape((n_small, features), f32), shape((n_dp * n_t, row_tiles, 128), f32), shape((rows, n_joined), f32),
        ],
        scratch_shapes=[pltpu.VMEM(*item) for item in scratch]
        + reduce_buffers(n_t, part, features, n_high) * 2
        + [pltpu.SemaphoreType.DMA((96,)), pltpu.SemaphoreType.DMA((96,)), pltpu.SemaphoreType.DMA((40,))],
        compiler_params=pltpu.CompilerParams(collective_id=1, has_side_effects=True, vmem_limit_bytes=67043328),
        name="backward",
    )(*small_inputs, *large_inputs)


def on_device(
    noisy_embed, self_cond, cond_flag, timestep, in_weight, qkv_weight, out_weight,
    up_weight, up_bias, down_weight, ada_weight, norm_gain, norm_bias, out_grad,
):
    n_t, tensor = lax.axis_size("tensor"), lax.axis_index("tensor")
    rows, features = out_grad.shape
    embed_cols = noisy_embed.shape[1]
    seq_len = rows * n_t // cond_flag.shape[0]
    assert seq_len == 2 * rows
    head_cols = qkv_weight.shape[2]
    hidden_cols = up_weight.shape[1]

    sequence = (tensor * rows) // seq_len
    flag = pick(cond_flag, sequence).astype(f32)
    embed_low = time_embed(lax.dynamic_slice_in_dim(timestep, sequence, 1, 0), ada_weight.shape[0]).astype(bf16)
    joined = jnp.concatenate([noisy_embed, (self_cond.astype(f32) * flag).astype(bf16)], axis=1)
    cosine, sine = rope_tables(seq_len, (tensor * rows) % seq_len)
    attn_quarter = jnp.concatenate([qkv_weight[0].T, qkv_weight[1].T, qkv_weight[2].T, out_weight])
    embed_rows = jnp.broadcast_to(embed_low, (16, embed_low.shape[1]))
    (
        result, joined_all, gate_row, ada, attn_all, ups, downs, attn_in, q, k, v, mixed, mixed_full, log_total,
        resid, modulated, act, slope, grad_branch,
    ) = forward(
        joined, up_bias.astype(f32)[None], (attn_quarter, up_weight, down_weight), in_weight, norm_gain[None],
        norm_bias[None], cosine, sine, embed_rows, ada_weight, out_grad,
    )
    grad_down, grad_up, grad_attn_w, small, ada_rows, grad_joined = backward(
        (
            joined_all, in_weight, norm_gain[None], cosine, sine, ada, gate_row, embed_rows, out_grad, grad_branch,
            modulated, resid,
        ),
        (act, slope, ups, downs, attn_all, q, k, v, mixed, mixed_full, log_total, attn_in),
        joined.shape[1],
    )
    grad_down = grad_down.reshape(hidden_cols, features).astype(f32)
    grad_up = grad_up.reshape(features, hidden_cols).astype(f32)
    grad_attn_w = grad_attn_w.reshape(4, head_cols, features).astype(f32)
    grad_qkv, grad_out = jnp.swapaxes(grad_attn_w[:3], 1, 2), grad_attn_w[3]
    ada_rows = ada_rows.reshape(ada_rows.shape[0], -1)
    grad_ada = lax.dot_general(
        ada_rows[:, 3 * features :], ada_rows[:, : 3 * features],
        (((0,), (0,)), ((), ())), precision=precise, preferred_element_type=f32,
    )
    grad_noisy = grad_joined[:, :embed_cols]
    grad_self = grad_joined[:, embed_cols:] * flag
    n_in = joined.shape[1]
    grad_in, grad_gain, grad_offset = small[:n_in], small[n_in], small[n_in + 1]
    grad_bias = pick(small[n_in + 2 : n_in + 2 + n_t].reshape(n_t, hidden_cols), tensor)
    return (
        result, grad_noisy, grad_self, grad_in, grad_qkv, grad_out, grad_up,
        grad_bias, grad_down, grad_ada, grad_gain, grad_offset,
    )


def solution(mesh):
    tokens = P(("dp", "tensor"), None)
    return jax.shard_map(
        on_device,
        mesh=mesh,
        in_specs=(
            tokens, tokens, P("dp"), P("dp"), P(), P(None, None, "tensor"), P("tensor", None),
            P(None, "tensor"), P("tensor"), P("tensor", None), P(), P(), P(), tokens,
        ),
        out_specs=(
            tokens, tokens, tokens, P(), P(None, None, "tensor"), P("tensor", None), P(None, "tensor"),
            P("tensor"), P("tensor", None), P(), P(), P(),
        ),
        check_vma=False,
    )
```

```python
import functools
import math

import jax
import jax.numpy as jnp
import numpy as np
from jax import lax
from jax.experimental import pallas as pl
from jax.experimental.pallas import tpu as pltpu
from jax.sharding import PartitionSpec as P

HD = 64
SPLIT = 8
norm_epsilon = 1e-05
precise = lax.Precision.HIGHEST
f32, bf16 = jnp.float32, jnp.bfloat16
MESH = pl.DeviceIdType.MESH


def nt(left, right):
    return lax.dot_general(left, right, (((1,), (1,)), ((), ())), preferred_element_type=f32)


def nn(left, right):
    return lax.dot_general(left, right, (((1,), (0,)), ((), ())), preferred_element_type=f32)


def tn(left, right):
    return lax.dot_general(left, right, (((0,), (0,)), ((), ())), preferred_element_type=f32)


def swap_halves(values):
    width = values.shape[1]
    lane = lax.broadcasted_iota(jnp.int32, values.shape, 1)
    return jnp.where(
        lane % HD < HD // 2,
        pltpu.roll(values, width - HD // 2, 1),
        pltpu.roll(values, HD // 2, 1),
    )


def norm_stats(values):
    center = jnp.mean(values, axis=-1, keepdims=True)
    spread = values - center
    second = jnp.mean(spread * spread, axis=-1, keepdims=True)
    inverse = lax.rsqrt(second + norm_epsilon)
    return spread * inverse, inverse


def norm_back(normed, inverse, upstream):
    first = jnp.mean(upstream, axis=-1, keepdims=True)
    cross = jnp.mean(upstream * normed, axis=-1, keepdims=True)
    return (upstream - first - normed * cross) * inverse


def rope_table(length):
    halfway = HD // 2
    freqs = np.exp(-np.float32(math.log(10000.0)) * np.arange(halfway, dtype=np.float32) * np.float32(2.0 / HD))
    angle = np.arange(length, dtype=np.float32)[:, None] * freqs[None, :].astype(np.float32)
    cosine, sine = np.cos(angle), np.sin(angle)
    return np.concatenate([np.tile(cosine, (1, 4)), np.tile(np.concatenate([-sine, sine], 1), (1, 2))], 1)


def time_embed(steps, channels):
    halfway = channels // 2
    freqs = jnp.exp(-math.log(10000.0) * jnp.arange(halfway, dtype=f32) * (1.0 / halfway))
    angle = steps.astype(f32)[:, None] * freqs[None, :]
    return jnp.concatenate([jnp.cos(angle), jnp.sin(angle)], axis=1)


def gelu_both(values):
    phi = 0.5 * (1.0 + lax.erf(values * math.sqrt(0.5)))
    bell = jnp.exp(-0.5 * values * values) * (1.0 / math.sqrt(2.0 * math.pi))
    return values * phi, phi + values * bell


def flip(index, bits):
    bit = 1
    while bit <= bits:
        if bits & bit:
            index = index + bit - 2 * bit * ((index // bit) % 2)
        bit *= 2
    return index


class Net:
    def __init__(self, n_dp, n_t, send_sems, recv_sems):
        self.dp, self.tensor = lax.axis_index("dp"), lax.axis_index("tensor")
        self.low = self.dp % SPLIT
        self.core, self.x, self.y = self.low % 2, (self.low // 2) % 2, self.low // 4
        self.n_t, self.high_bits = n_t, []
        while SPLIT << len(self.high_bits) < n_dp:
            self.high_bits.append(SPLIT << len(self.high_bits))
        self.sems, self.used = (send_sems, recv_sems), 0

    def peers(self):
        return [(b, 0) for b in [1, 2, 4] + self.high_bits] + [(0, k) for k in range(1, self.n_t)]

    def peer(self, bits):
        return {"dp": flip(self.dp, bits[0]), "tensor": flip(self.tensor, bits[1])}

    def barrier(self):
        ready = pltpu.get_barrier_semaphore()
        for bits in self.peers():
            pl.semaphore_signal(ready, inc=1, device_id=self.peer(bits), device_id_type=MESH)
        pl.semaphore_wait(ready, len(self.peers()))

    def send(self, source, target, bits):
        copy = pltpu.make_async_remote_copy(
            src_ref=source, dst_ref=target,
            send_sem=self.sems[0].at[self.used], recv_sem=self.sems[1].at[self.used],
            device_id=self.peer(bits), device_id_type=MESH,
        )
        self.used += 1
        return copy

    def local(self, source, target):
        copy = pltpu.make_async_copy(source, target, self.sems[0].at[self.used])
        self.used += 1
        return copy


def rows_of(piece, rows):
    return pl.ds(pl.multiple_of(piece * rows, rows), rows)


def start_all(*copies):
    for copy in copies:
        copy.start()


def arrived(*copies):
    for copy in copies:
        copy.wait_recv()


def sent(*copies):
    for copy in copies:
        copy.wait_send()


def loop(count, body):
    def step(i, carry):
        body(i)
        return carry

    lax.fori_loop(0, count, step, 0)


def run_steps(i, steps):
    for turn, act in steps:
        pl.when(i == turn)(act)


class Unit:
    def __init__(self, net, quarter, full, k):
        rows, half = quarter.shape[0] // SPLIT, quarter.shape[1] // 2
        mine, from_x, from_y, from_xy = (rows_of(flip(net.low, bits), rows) for bits in (0, 2, 4, 6))
        same = lambda view, bits: net.send(view, view, bits)
        self.by_z = net.send(quarter.at[mine], full.at[k, mine], (0, k))
        self.to_x, self.to_y = same(full.at[k, mine], (2, 0)), same(full.at[k, mine], (4, 0))
        self.x_to_y = same(full.at[k, from_x, pl.ds(0, half)], (4, 0))
        self.y_to_x = same(full.at[k, from_y, pl.ds(half, half)], (2, 0))
        self.to_core = [same(full.at[k, where], (1, 0)) for where in (mine, from_x, from_y, from_xy)]

    def begin(self):
        self.by_z.start()

    def plane(self):
        arrived(self.by_z)
        start_all(self.to_x, self.to_y, self.to_core[0])

    def relay(self):
        arrived(self.to_x)
        start_all(self.x_to_y, self.to_core[1])
        arrived(self.to_y)
        start_all(self.y_to_x, self.to_core[2])

    def across(self):
        arrived(self.x_to_y, self.y_to_x)
        self.to_core[3].start()

    def finish(self):
        arrived(*self.to_core)
        sent(self.by_z, self.to_x, self.to_y, self.x_to_y, self.y_to_x, *self.to_core)


class Collect:
    def __init__(self, net, out):
        parts = [(pl.ds(0, out.shape[-1] // 256 * 128),), (pl.ds(out.shape[-1] // 256 * 128, out.shape[-1] - out.shape[-1] // 256 * 128),)]
        full = (slice(None),) * (len(out.shape) - 2)
        mine, from_x, from_y, from_xy = (flip(net.low, bits) for bits in (0, 2, 4, 6))
        same = lambda view, bits: net.send(view, view, bits)
        self.to_x, self.to_y = same(out.at[mine], (2, 0)), same(out.at[mine], (4, 0))
        self.x_to_y = same(out.at[(from_x,) + full + parts[0]], (4, 0))
        self.y_to_x = same(out.at[(from_y,) + full + parts[1]], (2, 0))
        self.to_core = [same(out.at[where], (1, 0)) for where in (mine, from_x, from_y, from_xy)]

    def begin(self):
        start_all(self.to_x, self.to_y, self.to_core[0])

    def relay(self):
        arrived(self.to_x)
        start_all(self.x_to_y, self.to_core[1])
        arrived(self.to_y)
        start_all(self.y_to_x, self.to_core[2])

    def across(self):
        arrived(self.x_to_y, self.y_to_x)
        self.to_core[3].start()

    def finish(self):
        arrived(*self.to_core)
        sent(self.to_x, self.to_y, self.x_to_y, self.y_to_x, *self.to_core)


def half_buffers(blocks, rows, cols):
    shapes = [(blocks, 2, 2, rows, cols), (blocks, 2, rows, cols)] + [(blocks, rows, cols)] * 3
    return [pltpu.VMEM(shape, bf16) for shape in shapes]


class Half:
    def __init__(self, net, terms, buffers, x_first, groups):
        self.net, self.terms, self.x_first = net, terms, x_first
        self.came, self.first, self.second, self.total, self.away = buffers
        self.blocks = terms.shape[0]
        c, near, far = net.core, (2, 0), (4, 0)
        if not x_first:
            near, far = far, near
        self.there = [net.send(terms.at[b, :, :, 1 - c], self.came.at[b], (1, 0)) for b in range(self.blocks)]
        theirs = terms.at[:, :, 1 - net.x, c] if x_first else terms.at[:, 1 - net.y, :, c]
        self.one = net.send(theirs, self.first, near)
        other = 1 - net.y if x_first else 1 - net.x
        self.two = net.send(self.first.at[:, other], self.second, far)
        self.three = [
            net.send(self.total.at[where], self.away.at[where], (0, k)) for k, where in groups if k
        ]

    def begin(self, block):
        self.there[block].start()

    def add_core(self):
        arrived(*self.there)
        terms, came, c = self.terms, self.came, self.net.core

        def add(i):
            b, y, x = i // 4, (i // 2) % 2, i % 2
            terms[b, y, x, c] = (terms[b, y, x, c].astype(f32) + came[b, y, x].astype(f32)).astype(bf16)

        loop(4 * self.blocks, add)
        self.one.start()

    def add_first(self):
        arrived(self.one)
        net, terms, first, c = self.net, self.terms, self.first, self.net.core

        def add(i):
            b, j = i // 2, i % 2
            mine = terms[b, j, net.x, c] if self.x_first else terms[b, net.y, j, c]
            first[b, j] = (mine.astype(f32) + first[b, j].astype(f32)).astype(bf16)

        loop(2 * self.blocks, add)
        self.two.start()
        sent(*self.there, self.one)

    def add_second(self):
        arrived(self.two)
        here = self.net.y if self.x_first else self.net.x

        def add(b):
            self.total[b] = (self.first[b, here].astype(f32) + self.second[b].astype(f32)).astype(bf16)

        loop(self.blocks, add)
        start_all(*self.three)
        sent(self.two)

    def close(self):
        arrived(*self.three)
        sent(*self.three)


def both(halves, name):
    def step():
        for half in halves:
            getattr(half, name)()

    return step


def add_high(net, copies, more, out, total):
    for n, copy in enumerate(copies):
        out[net.low] = total.astype(bf16)
        copy.start()
        arrived(copy)
        sent(copy)
        total = total + more[n].astype(f32)
    return total


def high_copies(net, more, out):
    return [net.send(out.at[net.low], more.at[n], (bit, 0)) for n, bit in enumerate(net.high_bits)]


ANY = pl.BlockSpec(memory_space=pl.ANY)
VMEM = pl.BlockSpec(memory_space=pltpu.VMEM)
SMEM = pl.BlockSpec(memory_space=pltpu.SMEM)


def forward_kernel(
    n_dp, n_t,
    flag_ref, noisy_ref, self_ref, pack_ref, a_ref, u_ref, d_ref, in_ref, table_ref, embed_ref, ada_ref, og_ref,
    result_ref, joined_ref, row_ref, ada_row_ref,
    a_out, u_out, d_out, attn_out, q_out, k_out, v_out, m_out, mf_out, l_out,
    resid_out, mod_out, act_out, slope_out, gb_out,
    a_s, u_s, d_s, attn_in, q_s, k_s, v_s, m_s, mf_s, l_s, resid, mod_s, act_s, slope_s, gb_s,
    joined_s, bias_s, branch, hidden, send_sems, recv_sems,
):
    net = Net(n_dp, n_t, send_sems, recv_sems)
    rows, features = og_ref.shape
    length, head_cols, n_pairs = joined_s.shape[0], features // n_t, features // 128
    others = range(1, n_t)
    a = [None] + [Unit(net, a_ref, a_s, k) for k in others]
    u = [None] + [Unit(net, u_ref, u_s, k) for k in others]
    d = [None] + [Unit(net, d_ref, d_s, k) for k in others]
    own_copies = [net.local(quarter, full.at[0]) for quarter, full in ((a_ref, a_s), (u_ref, u_s), (d_ref, d_s))]
    own, far = pl.ds(0, rows), pl.ds(rows, rows)
    joined_copy = net.send(joined_s.at[own], joined_s.at[far], (0, 1))
    bias_copies = [net.send(bias_s.at[0], bias_s.at[k], (0, k)) for k in others]
    kept = [
        net.local(source, target)
        for source, target in (
            (attn_in, attn_out), (q_s, q_out), (k_s, k_out), (v_s, v_out), (m_s, m_out),
            (mf_s, mf_out), (l_s, l_out), (resid, resid_out), (mod_s, mod_out), (act_s, act_out),
            (slope_s, slope_out), (gb_s, gb_out), (a_s, a_out), (u_s, u_out), (d_s, d_out),
        )
    ]
    sequence = net.tensor // 2
    joined_s[own, :] = jnp.concatenate(
        [noisy_ref[...], (self_ref[...].astype(f32) * flag_ref[sequence].astype(f32)).astype(bf16)], axis=1
    )
    bias_s[0] = pack_ref[2:3, :]
    gain, offset = pack_ref[0:1, :], pack_ref[1:2, :]
    net.barrier()
    for unit in a[1:]:
        unit.begin()
    start_all(joined_copy, *bias_copies, *own_copies)
    chunk = 256

    def norm_rows(i, mine):
        where = pl.ds(pl.multiple_of(i * chunk, chunk), chunk)
        values = nn(joined_s[where, :], in_ref[...])
        if mine:
            hidden[where, :] = values
        attn_in[where, :] = (norm_stats(values)[0] * gain + offset).astype(bf16)

    per = rows // chunk
    loop(per, lambda i: norm_rows(i, True))
    a[1].plane()
    u[1].begin()
    line = lax.broadcasted_iota(jnp.int32, (embed_ref.shape[0], 1), 0) == sequence
    ada = jnp.sum(jnp.where(line, nn(embed_ref[...], ada_ref[...]), 0.0), axis=0, keepdims=True)
    ada_row_ref[...] = ada
    row_ref[:, features:] = jnp.sum(jnp.where(line, embed_ref[...].astype(f32), 0.0), axis=0, keepdims=True)
    shift, scale, gate = ada[:, :features], 1.0 + ada[:, features : 2 * features], ada[:, 2 * features :]
    a[2].plane()
    u[2].begin()
    arrived(joined_copy)
    joined_ref[...] = joined_s[...]
    loop(per, lambda i: norm_rows(i + per, False))
    a[3].plane()
    u[3].begin()
    a[1].relay()
    a[2].relay()
    a[1].across()
    a[3].relay()
    a[2].across()
    u[1].plane()
    d[1].begin()
    a[3].across()
    u[2].plane()
    d[2].begin()
    a[1].finish()
    own_copies[0].wait()
    u[3].plane()
    d[3].begin()
    a[2].finish()
    a[3].finish()

    def project(i):
        wide = 2 * head_cols
        weight = lambda m: a_s[pl.ds(2 * i, 2), pl.ds(m * head_cols, head_cols), :].reshape(wide, features)

        def rotated(proj, first):
            spot = pl.ds(pl.multiple_of(first, rows), rows)
            cosine = jnp.concatenate([table_ref[spot, 0:128]] * (wide // 128), axis=1)
            sine = jnp.concatenate([table_ref[spot, 128:256]] * (wide // 128), axis=1)
            return proj * cosine + swap_halves(proj) * sine

        own_first = (net.tensor % 2) * rows
        far_first = rows - own_first
        query = (rotated(nt(attn_in[own, :], weight(0)), own_first) * HD**-0.5).astype(bf16)
        key_own = rotated(nt(attn_in[own, :], weight(1)), own_first).astype(bf16)
        key_far = rotated(nt(attn_in[far, :], weight(1)), far_first).astype(bf16)
        value = nt(attn_in[...], weight(2)).astype(bf16)
        for pair in range(wide // 128):
            where = i * (wide // 128) + pair
            cols = slice(pair * 128, (pair + 1) * 128)
            q_s[where], v_s[where] = query[:, cols], value[:, cols]
            k_s[where, own, :], k_s[where, far, :] = key_own[:, cols], key_far[:, cols]

    def project_step(i):
        project(i)
        pl.when(i == 0)(u[1].relay)

    loop(n_t // 2, project_step)
    lane = lax.broadcasted_iota(jnp.int32, (rows, 128), 1)

    def attend(pair):
        keys, values, queries = k_s[pair], v_s[pair], q_s[pair]
        out = stat = None
        for head in range(2):
            scores = nt(jnp.where(lane // HD == head, queries, jnp.zeros_like(queries)), keys)
            top = jnp.max(scores, axis=1, keepdims=True)
            probs = jnp.exp(scores - top)
            total = jnp.sum(probs, axis=1, keepdims=True)
            mixed = nn(probs.astype(bf16), values) * (1.0 / total)
            log_total = jnp.broadcast_to(top + jnp.log(total), (rows, 128))
            out = mixed if head == 0 else jnp.where(lane < HD, out, mixed)
            stat = log_total if head == 0 else jnp.where(lane < HD, stat, log_total)
        m_s[:, pl.ds(pl.multiple_of(pair * 128, 128), 128)] = out.astype(bf16)
        mf_s[pair] = out
        l_s[pair] = stat

    steps = [
        (0, u[2].relay), (0, u[1].across), (1, u[3].relay), (1, d[1].plane), (1, u[2].across), (2, d[2].plane),
        (2, u[3].across), (2, u[1].finish), (3, d[3].plane), (3, d[1].relay), (3, u[2].finish), (4, d[2].relay),
        (4, d[1].across), (5, d[3].relay), (5, d[2].across), (5, u[3].finish),
    ]

    def attend_step(i):
        attend(i)
        run_steps(i, steps)

    loop(n_pairs, attend_step)
    start_all(*kept[:7], kept[12])
    out_weight = a_s[:, pl.ds(3 * head_cols, head_cols), :].reshape(features, features)
    resid[...] = hidden[...] + nn(m_s[...], out_weight)

    def norm_again(i):
        where = pl.ds(pl.multiple_of(i * chunk, chunk), chunk)
        mod_s[where, :] = (scale * norm_stats(resid[where, :])[0] + shift).astype(bf16)
        gb_s[where, :] = (gate * og_ref[where, :]).astype(bf16)

    loop(per, norm_again)
    arrived(*bias_copies)
    own_copies[1].wait()
    d[3].across()
    start_all(kept[7], kept[8], kept[11], kept[13])
    branch[...] = jnp.zeros_like(branch)

    def up(i):
        k, where = i // 2, pl.ds(pl.multiple_of((i % 2) * (rows // 2), rows // 2), rows // 2)
        pre = nn(mod_s[where, :], u_s[k]) + bias_s[k]
        act, slope = gelu_both(pre)
        act_s[k, where, :] = act.astype(bf16)
        slope_s[k, where, :] = slope.astype(bf16)

    loop(2 * n_t, up)
    start_all(kept[9], kept[10])
    own_copies[2].wait()
    for unit in d[1:]:
        unit.finish()
    kept[14].start()

    def down(k):
        branch[...] += nn(act_s[k], d_s[k])

    loop(n_t, down)
    result_ref[...] = resid[...] + gate * branch[...]
    row_ref[:, :features] = jnp.sum(og_ref[...] * branch[...], axis=0, keepdims=True)
    for copy in kept:
        copy.wait()
    sent(joined_copy, *bias_copies)


def forward(flags, noisy, self_cond, pack, quarters, in_weight, table, embed, ada_weight, out_grad):
    n_dp, n_t = lax.axis_size("dp"), lax.axis_size("tensor")
    (rows, features), length = out_grad.shape, 2 * out_grad.shape[0]
    pairs, hidden_cols, n_joined = features // 128, quarters[1].shape[1], 2 * noisy.shape[1]
    shape = jax.ShapeDtypeStruct
    kept = [((n_t,) + w.shape, bf16) for w in quarters] + [
        ((length, features), bf16),
        ((pairs, rows, 128), bf16), ((pairs, length, 128), bf16), ((pairs, length, 128), bf16),
        ((rows, features), bf16), ((pairs, rows, 128), f32), ((pairs, rows, 128), f32),
        ((rows, features), f32), ((rows, features), bf16),
        ((n_t, rows, hidden_cols), bf16), ((n_t, rows, hidden_cols), bf16), ((rows, features), bf16),
    ]
    scratch = kept + [
        ((length, n_joined), bf16), ((n_t, 1, hidden_cols), f32), ((rows, features), f32), ((rows, features), f32),
    ]
    return pl.pallas_call(
        functools.partial(forward_kernel, n_dp, n_t),
        in_specs=[SMEM] + [VMEM] * 11,
        out_specs=[VMEM] * 4 + [ANY] * len(kept),
        out_shape=[
            shape((rows, features), f32), shape((length, n_joined), bf16),
            shape((1, features + ada_weight.shape[0]), f32), shape((1, ada_weight.shape[1]), f32),
        ] + [shape(*item) for item in kept],
        scratch_shapes=[pltpu.VMEM(*item) for item in scratch] + [pltpu.SemaphoreType.DMA((128,))] * 2,
        compiler_params=pltpu.CompilerParams(collective_id=0, has_side_effects=True, vmem_limit_bytes=67043328),
        name="forward",
    )(flags, noisy, self_cond, pack, *quarters, in_weight, table, embed, ada_weight, out_grad)


def backward_kernel(
    n_dp, n_t,
    flag_ref, joined_ref, in_ref, pack_ref, table_ref, ada_ref, row_ref, og_ref, gb_ref, mod_ref, resid_ref,
    act_ref, slope_ref, u_ref, d_ref, a_ref, q_ref, k_ref, v_ref, m_ref, mf_ref, l_ref, attn_ref,
    d_out, u_out, o_out, q_out, small_out, rows_out, gj_out,
    terms_d, terms_u, terms_o, terms_q, act_b, slope_b, d_b, u_b, grad, grad_low, q_b, k_b, v_b, mf_b, l_b,
    dk_s, dv_s, acc_k, acc_v, small_b, gj_far, row_s, more_d, more_u, more_o, more_q, *scratch,
):
    send_sems, recv_sems, load_sems = scratch[-3:]
    net = Net(n_dp, n_t, send_sems, recv_sems)
    rows, features = og_ref.shape
    length, head_cols = joined_ref.shape[0], features // n_t
    n_pairs, chunk, n_in, mid = features // 128, 256, joined_ref.shape[1], n_t // 2
    spare = iter(scratch[:-3])
    half = lambda terms, x_first, groups: Half(net, terms, [next(spare) for _ in range(5)], x_first, groups)
    each = lambda ks: [(k, pl.ds(n, 1)) for n, k in enumerate(ks)]
    d = [half(terms_d.at[i], i == 0, each(range(n_t))) for i in range(2)]
    u = [half(terms_u.at[i], i == 0, each(range(n_t))) for i in range(2)]
    o = [half(terms_o.at[i], i == 0, each(range(i * mid, (i + 1) * mid))) for i in range(2)]
    kinds = pl.ds(0, 3)
    q_far = [half(terms_q.at[0, i], i == 0, [(mid + i, kinds)]) for i in range(2)]
    q_near = [half(terms_q.at[1, i], i == 0, [(i, kinds)]) for i in range(2)]
    d_all, u_all, o_all, q_all = (Collect(net, out) for out in (d_out, u_out, o_out, q_out))
    highs = [
        high_copies(net, more, out)
        for more, out in ((more_d, d_out), (more_u, u_out), (more_o, o_out), (more_q, q_out))
    ]

    def close_ff(halves, out, high, more, collect):
        def step():
            parts = []
            for one in halves:
                one.close()
                total = one.total[0].astype(f32)
                for k in range(1, n_t):
                    total = total + one.away[k].astype(f32)
                parts.append(total)
            out[net.low] = add_high(net, high, more, out, jnp.concatenate(parts, axis=1)).astype(bf16)
            collect.begin()

        return step

    def close_o():
        for one in o:
            one.close()
        total = o[0].total[0].astype(f32) + o[0].away[1].astype(f32) + o[1].away[0].astype(f32)
        total = total + o[1].away[1].astype(f32)
        o_out[net.low] = add_high(net, highs[2], more_o, o_out, total).astype(bf16)
        o_all.begin()

    def close_q():
        for one in q_far + q_near:
            one.close()
        total = q_near[0].total[...].astype(f32)
        for one in (q_near[1], q_far[0], q_far[1]):
            total = total + one.away[...].astype(f32)
        q_out[net.low] = add_high(net, highs[3], more_q, q_out, total).astype(bf16)
        q_all.begin()

    close_d = close_ff(d, d_out, highs[0], more_d, d_all)
    close_u = close_ff(u, u_out, highs[1], more_u, u_all)

    def stream(first_sem, order, *pairs):
        copies = lambda i: [
            pltpu.make_async_copy(source.at[order(i)], target.at[i % 2], load_sems.at[first_sem + 2 * n + i % 2])
            for n, (source, target) in enumerate(pairs)
        ]
        return (lambda i: start_all(*copies(i))), (lambda i: [copy.wait() for copy in copies(i)])

    same = lambda i: i
    act_start, act_wait = stream(0, same, (act_ref, act_b))
    ff_start, ff_wait = stream(2, same, (slope_ref, slope_b), (d_ref, d_b), (u_ref, u_b))
    pair_of = lambda i: (i + n_pairs // 2) % n_pairs
    at_start, at_wait = stream(8, pair_of, (q_ref, q_b), (k_ref, k_b), (v_ref, v_b), (mf_ref, mf_b), (l_ref, l_b))
    load_m = pltpu.make_async_copy(m_ref, slope_b.at[0], load_sems.at[18])
    load_attn = [
        pltpu.make_async_copy(attn_ref.at[pl.ds(i * rows, rows)], act_b.at[i], load_sems.at[19 + i]) for i in range(2)
    ]
    weights = [(d_b, 0), (d_b, 1), (u_b, 0), (u_b, 1)]
    load_w = [
        [
            pltpu.make_async_copy(
                a_ref.at[k, pl.ds(m * head_cols, head_cols)], ref.at[slot, pl.ds(k * head_cols, head_cols)],
                load_sems.at[21 + m * n_t + k],
            )
            for k in range(n_t)
        ]
        for m, (ref, slot) in enumerate(weights)
    ]
    load_row = pltpu.make_async_copy(row_s, rows_out.at[pl.ds(0, 1)], load_sems.at[37])
    bits = [(0, 1 << b) for b in range((n_t - 1).bit_length())] + [(b, 0) for b in [1, 2, 4] + net.high_bits]
    row_copies = [
        net.send(rows_out.at[pl.ds(0, 1 << n)], rows_out.at[pl.ds(1 << n, 1 << n)], bit) for n, bit in enumerate(bits)
    ]
    sum_copies = [net.send(small_b.at[0], small_b.at[n + 1], bit) for n, bit in enumerate(bits)]
    gj_s = acc_k
    gj_copy = net.send(gj_s.at[pl.ds(rows, rows)], gj_far, (0, 1))

    def row_step(n):
        def step():
            if n:
                arrived(row_copies[n - 1])
            if n < len(bits):
                row_copies[n].start()

        return step

    def sum_step(n):
        def step():
            if n == 0:
                sum_copies[0].start()
                return
            arrived(sum_copies[n - 1])
            sent(sum_copies[n - 1])
            total = small_b[0] + small_b[n]
            if n < len(bits):
                small_b[0] = total
                sum_copies[n].start()
            else:
                small_out[...] = total

        return step

    act_start(0)
    ff_start(0)
    net.barrier()
    scale = 1.0 + ada_ref[:, features : 2 * features]
    gb = gb_ref[...]
    wide = features // 2

    def store_ff(terms, k, values):
        for i in range(2):
            terms[i, k] = values[:, i * wide : (i + 1) * wide].reshape(terms.shape[2:])

    def begin(halves, block):
        for one in halves:
            one.begin(block)

    def down_terms(k):
        pl.when(k + 1 < n_t)(lambda: act_start(k + 1))
        act_wait(k)
        store_ff(terms_d, k, tn(act_b[k % 2], gb).astype(bf16))
        run_steps(k, [(turn, functools.partial(begin, d, turn)) for turn in range(n_t)])

    loop(n_t, down_terms)
    start_all(*load_attn)
    grad[...] = jnp.zeros_like(grad)
    small_b[0] = jnp.zeros(small_b.shape[1:], f32)

    def ff_back(k):
        pl.when(k + 1 < n_t)(lambda: ff_start(k + 1))
        ff_wait(k)
        slot = k % 2
        grad_pre = (slope_b[slot].astype(f32) * nt(gb, d_b[slot])).astype(bf16)
        place = n_in + 2 + net.tensor
        bit = 1
        while bit < n_t:
            place = place + jnp.where((k // bit) % 2 == 1, flip(net.tensor, bit) - net.tensor, 0)
            bit *= 2
        small_b[0, pl.ds(place, 1), :] = jnp.sum(grad_pre.astype(f32), axis=0, keepdims=True)
        store_ff(terms_u, k, tn(mod_ref[...], grad_pre).astype(bf16))
        run_steps(
            k, [(turn, functools.partial(begin, u, turn)) for turn in range(n_t)] + [(0, both(d, "add_core"))]
        )
        grad[...] += nt(grad_pre, u_b[slot])

    loop(n_t, ff_back)
    load_m.start()
    for copies in load_w[::-1]:
        start_all(*copies)
    at_start(0)
    shift_row = scale_row = 0.0
    for i in range(rows // chunk):
        where = pl.ds(i * chunk, chunk)
        upstream = grad[where, :]
        normed, inverse = norm_stats(resid_ref[where, :])
        shift_row += jnp.sum(upstream, axis=0, keepdims=True)
        scale_row += jnp.sum(upstream * normed, axis=0, keepdims=True)
        total = og_ref[where, :] + norm_back(normed, inverse, scale * upstream)
        grad[where, :] = total
        grad_low[where, :] = total.astype(bf16)
    row = jnp.concatenate([shift_row, scale_row, row_ref[...]], axis=1)
    for i in range(row.shape[1] // 128):
        row_s[0, i : i + 1, :] = row[:, i * 128 : (i + 1) * 128]
    load_row.start()
    load_row.wait()
    row_step(0)()
    load_m.wait()
    for copy in load_w[3]:
        copy.wait()
    def store_heads(terms, values):
        part = head_cols // (SPLIT // 2)
        for j in range(SPLIT // 2):
            for c in range(2):
                terms[j // 2, j % 2, c] = values[j * part : (j + 1) * part, c * wide : (c + 1) * wide]

    join = lambda ref, where, first=0, count=n_pairs: jnp.concatenate(
        [ref[first + pair, where, :] for pair in range(count)], axis=1
    )
    own, every = pl.ds(0, rows), pl.ds(0, length)
    out_terms = tn(slope_b[0], grad_low[...]).astype(bf16)
    for k in range(n_t):
        store_heads(terms_o.at[k // mid, k % mid], out_terms[k * head_cols : (k + 1) * head_cols])
    grad_low[...] = nt(grad_low[...], u_b[1]).astype(bf16)
    both(d, "add_first")()
    both(u, "add_core")()
    for block in range(mid):
        begin(o, block)

    def rotated_back(values, first):
        spot = pl.ds(pl.multiple_of(first, rows), rows)
        return values * table_ref[spot, 0:128] + swap_halves(values * table_ref[spot, 128:256])

    own_first = (net.tensor % 2) * rows

    def attend_back(i):
        pl.when(i + 1 < n_pairs)(lambda: at_start(i + 1))
        at_wait(i)
        slot, pair = i % 2, pair_of(i)
        cols = pl.ds(pl.multiple_of(pair * 128, 128), 128)
        keys, values, queries, grads = k_b[slot], v_b[slot], q_b[slot], grad_low[:, cols]
        lane = lax.broadcasted_iota(jnp.int32, queries.shape, 1)
        product = grads.astype(f32) * mf_b[slot]
        grad_q = None
        for head in range(2):
            mine = lane // HD == head
            q_head = jnp.where(mine, queries, jnp.zeros_like(queries))
            g_head = jnp.where(mine, grads, jnp.zeros_like(grads))
            center = jnp.sum(jnp.where(mine, product, 0.0), axis=1, keepdims=True)
            probs = jnp.exp(nt(q_head, keys) - l_b[slot, :, pl.ds(head * HD, 1)])
            grad_prob = nt(g_head, values)
            grad_score = (probs * (grad_prob - center)).astype(bf16)
            part = nn(grad_score, keys) * HD**-0.5
            grad_q = part if head == 0 else jnp.where(lane < HD, grad_q, part)
            part_v = tn(probs.astype(bf16), g_head)
            part_k = tn(grad_score, q_head)
            if head == 0:
                acc_k[...] = part_k
                acc_v[...] = part_v
            else:
                dk = acc_k[...] + part_k
                dv = acc_v[...] + part_v
        grad_low[:, cols] = rotated_back(grad_q, own_first).astype(bf16)
        dk_s[pair, own, :] = rotated_back(dk[:rows], own_first).astype(bf16)
        dk_s[pair, pl.ds(rows, rows), :] = rotated_back(dk[rows:], rows - own_first).astype(bf16)
        dv_s[pair] = dv.astype(bf16)

    def head_terms(side):
        first, count = (1 - side) * (n_pairs // 2), n_pairs // 2
        for m, ref in enumerate((None, dk_s, dv_s)):
            if m == 0:
                columns = pl.ds(pl.multiple_of(first * 128, 128), count * 128)
                values = tn(grad_low[:, columns], act_b[0]).astype(bf16)
            else:
                values = tn(join(ref, every, first, count), act_b[...].reshape(length, features)).astype(bf16)
            for i in range(mid):
                store_heads(terms_q.at[side, i, m], values[i * head_cols : (i + 1) * head_cols])

    def launch_far():
        for m in range(3):
            begin(q_far, m)

    steps = [
        (0, both(o, "add_core")), (1, both(d, "add_second")), (2, both(u, "add_first")), (2, both(o, "add_first")),
        (3, both(q_far, "add_core")), (3, both(o, "add_second")), (4, both(u, "add_second")), (4, close_d),
        (5, both(q_far, "add_first")), (5, d_all.relay), (5, close_o),
    ]
    steps += [(min(n, n_pairs - 1), row_step(n + 1)) for n in range(len(bits))]
    for copy in load_attn:
        copy.wait()

    def attend_side(side):
        def pair_step(n):
            i = side * (n_pairs // 2) + n
            attend_back(i)
            run_steps(i, steps)

        loop(n_pairs // 2, pair_step)
        head_terms(side)
        pl.when(side == 0)(launch_far)

    loop(2, attend_side)
    for m in range(3):
        begin(q_near, m)
    both(q_far, "add_second")()
    d_all.across()
    o_all.relay()
    for copies in load_w[:3]:
        for copy in copies:
            copy.wait()

    def norm_grads(i, mine):
        where = pl.ds(pl.multiple_of(i * chunk, chunk), chunk)
        tokens = joined_ref[where, :]
        normed, inverse = norm_stats(nn(tokens, in_ref[...]))
        total = nn(join(dk_s, where), d_b[1]) + nn(join(dv_s, where), u_b[0])
        if mine:
            total = total + nn(grad_low[where, :], d_b[0])
        small_b[0, n_in : n_in + 1, :] += jnp.sum(total * normed, axis=0, keepdims=True)
        small_b[0, n_in + 1 : n_in + 2, :] += jnp.sum(total, axis=0, keepdims=True)
        upstream = norm_back(normed, inverse, total * pack_ref[0:1, :])
        if mine:
            upstream = upstream + grad[where, :]
        upstream = upstream.astype(bf16)
        small_b[0, 0:n_in, :] += tn(tokens, upstream)
        gj_s[where, 0:n_in] = nt(upstream, in_ref[...])

    per = rows // chunk
    both(q_near, "add_core")()
    loop(per, lambda i: norm_grads(i + per, False))
    gj_copy.start()
    close_u()
    o_all.across()
    loop(per, lambda i: norm_grads(i, True))
    sums = [sum_step(n) for n in range(len(bits) + 1)]
    sums.pop(0)()
    tail = [
        both(q_near, "add_first"), u_all.relay, both(q_near, "add_second"), u_all.across, close_q, q_all.relay,
        q_all.across,
    ]
    for n in range(max(len(tail), len(sums))):
        if n < len(tail):
            tail[n]()
        if n < len(sums):
            sums[n]()
    arrived(gj_copy)
    keep = jnp.where(lax.broadcasted_iota(jnp.int32, (rows, n_in), 1) < n_in // 2, 1.0, flag_ref[net.tensor // 2].astype(f32))
    gj_out[...] = (gj_s[own, 0:n_in] + gj_far[:, 0:n_in]) * keep
    for collect in (d_all, o_all, u_all, q_all):
        collect.finish()
    sent(gj_copy, *row_copies)


def backward(small_inputs, large_inputs):
    n_dp, n_t = lax.axis_size("dp"), lax.axis_size("tensor")
    joined, ada, row, og = small_inputs[1], small_inputs[5], small_inputs[6], small_inputs[7]
    (rows, features), (length, n_joined) = og.shape, joined.shape
    hidden_cols, head_cols = large_inputs[2].shape[2], features // n_t
    pairs, n_high = features // 128, (n_dp // SPLIT).bit_length() - 1
    n_bits = (n_dp * n_t).bit_length() - 1
    n_small = -(-(n_joined + 2 + n_t) // 8) * 8
    row_tiles = (ada.shape[1] - features + row.shape[1]) // 128
    shape = jax.ShapeDtypeStruct
    part, wide, mid, piece = features // SPLIT, features // 2, n_t // 2, head_cols // (SPLIT // 2)
    outs = [(part, features), (part, features), (piece, wide), (3, piece, wide)]
    scratch = [
        ((2, n_t, 2, 2, 2, part, wide), bf16), ((2, n_t, 2, 2, 2, part, wide), bf16),
        ((2, mid, 2, 2, 2, piece, wide), bf16), ((2, 2, 3, 2, 2, 2, piece, wide), bf16),
        ((2, rows, hidden_cols), bf16), ((2, rows, hidden_cols), bf16),
        ((2, hidden_cols, features), bf16), ((2, features, hidden_cols), bf16), ((rows, features), f32),
        ((rows, features), bf16),
        ((2, rows, 128), bf16), ((2, length, 128), bf16), ((2, length, 128), bf16), ((2, rows, 128), f32),
        ((2, rows, 128), f32),
        ((pairs, length, 128), bf16), ((pairs, length, 128), bf16),
        ((length, 128), f32), ((length, 128), f32), ((n_bits + 1, n_small, features), f32),
        ((rows, 128), f32), ((1, row_tiles, 128), f32),
    ] + [((max(n_high, 1),) + (out if n_high else (16, 128)), bf16) for out in outs]
    halves = []
    for blocks, r in ((n_t, part),) * 4 + ((mid, piece),) * 2 + ((3, piece),) * 4:
        halves += half_buffers(blocks, r, wide)
    return pl.pallas_call(
        functools.partial(backward_kernel, n_dp, n_t),
        in_specs=[SMEM] + [VMEM] * (len(small_inputs) - 1) + [ANY] * len(large_inputs),
        out_specs=[VMEM] * 5 + [ANY, VMEM],
        out_shape=[shape((SPLIT,) + out, bf16) for out in outs]
        + [
            shape((n_small, features), f32), shape((n_dp * n_t, row_tiles, 128), f32), shape((rows, n_joined), f32),
        ],
        scratch_shapes=[pltpu.VMEM(*item) for item in scratch]
        + halves
        + [pltpu.SemaphoreType.DMA((160,)), pltpu.SemaphoreType.DMA((160,)), pltpu.SemaphoreType.DMA((40,))],
        compiler_params=pltpu.CompilerParams(collective_id=1, has_side_effects=True, vmem_limit_bytes=67043328),
        name="backward",
    )(*small_inputs, *large_inputs)


def on_device(
    noisy_embed, self_cond, cond_flag, timestep, in_weight, qkv_weight, out_weight,
    up_weight, up_bias, down_weight, ada_weight, norm_gain, norm_bias, out_grad,
):
    n_t, tensor = lax.axis_size("tensor"), lax.axis_index("tensor")
    rows, features = out_grad.shape
    embed_cols = noisy_embed.shape[1]
    seq_len = rows * n_t // cond_flag.shape[0]
    assert seq_len == 2 * rows and n_t == 4
    head_cols, hidden_cols = qkv_weight.shape[2], up_weight.shape[1]
    assert hidden_cols == features

    table = jnp.asarray(rope_table(seq_len), f32)
    pack = jnp.stack([norm_gain, norm_bias, up_bias.astype(f32)])
    embed = time_embed(timestep, ada_weight.shape[0]).astype(bf16)
    embed = jnp.concatenate([embed, jnp.zeros((16 - embed.shape[0], embed.shape[1]), bf16)])
    attn_quarter = jnp.concatenate([qkv_weight[0].T, qkv_weight[1].T, qkv_weight[2].T, out_weight])
    (
        result, joined, row, ada, attn_all, ups, downs, attn_in, q, k, v, mixed, mixed_full, log_total,
        resid, modulated, act, slope, grad_branch,
    ) = forward(
        cond_flag, noisy_embed, self_cond, pack, (attn_quarter, up_weight, down_weight), in_weight, table, embed,
        ada_weight, out_grad,
    )
    grad_down, grad_up, grad_out, grad_qkv, small, ada_rows, grad_joined = backward(
        (cond_flag, joined, in_weight, pack, table, ada, row, out_grad, grad_branch, modulated, resid),
        (act, slope, ups, downs, attn_all, q, k, v, mixed, mixed_full, log_total, attn_in),
    )
    grad_down = grad_down.reshape(hidden_cols, features).astype(f32)
    grad_up = grad_up.reshape(features, hidden_cols).astype(f32)
    grad_out = grad_out.reshape((SPLIT // 2, 2) + grad_out.shape[1:])
    grad_out = jnp.transpose(grad_out, (0, 2, 1, 3)).reshape(head_cols, features).astype(f32)
    grad_qkv = grad_qkv.reshape((SPLIT // 2, 2) + grad_qkv.shape[1:])
    grad_qkv = jnp.transpose(grad_qkv, (2, 1, 4, 0, 3)).reshape(3, features, head_cols).astype(f32)
    ada_rows = ada_rows.reshape(ada_rows.shape[0], -1)
    grad_ada = lax.dot_general(
        ada_rows[:, 3 * features :], ada_rows[:, : 3 * features],
        (((0,), (0,)), ((), ())), precision=precise, preferred_element_type=f32,
    )
    n_in = in_weight.shape[0]
    grad_bias = lax.dynamic_index_in_dim(small, n_in + 2 + tensor, 0, keepdims=False)
    return (
        result, grad_joined[:, :embed_cols], grad_joined[:, embed_cols:], small[:n_in], grad_qkv, grad_out, grad_up,
        grad_bias, grad_down, grad_ada, small[n_in], small[n_in + 1],
    )


def solution(mesh):
    tokens = P(("dp", "tensor"), None)
    return jax.shard_map(
        on_device,
        mesh=mesh,
        in_specs=(
            tokens, tokens, P("dp"), P("dp"), P(), P(None, None, "tensor"), P("tensor", None),
            P(None, "tensor"), P("tensor"), P("tensor", None), P(), P(), P(), tokens,
        ),
        out_specs=(
            tokens, tokens, tokens, P(), P(None, None, "tensor"), P("tensor", None), P(None, "tensor"),
            P("tensor"), P("tensor", None), P(), P(), P(),
        ),
        check_vma=False,
    )
```
